32 devices in a mesh: dp: 2 (over x), seq: 4 (over z), tensor: 4 (over y, core).
Axes of the slice: x: 2, y: 2, z: 4, core: 2. Of those that a mesh axis runs over, the one named last changes fastest.
Arguments:
- block_input: bfloat16 [4096, 4, 1536], P(('seq', 'tensor'), 'dp'), may hold values from -6 to 6
- gain_in: float32 [1536], replicated, may hold values from 0.1 to 1.9
- w_zx: bfloat16 [1536, 2, 3072], P(('dp', 'seq'), None, 'tensor'), may hold values from -0.15625 to 0.15625
- w_bc: bfloat16 [1536, 2, 128], P(('dp', 'seq')), may hold values from -0.15625 to 0.15625
- w_dt: bfloat16 [1536, 48], P(('dp', 'seq'), 'tensor'), may hold values from -0.15625 to 0.15625
- conv_x: float32 [4, 3072], P(None, 'tensor'), may hold values from -3 to 3
- conv_x_b: float32 [3072], P('tensor'), may hold values from -0.5 to 0.5
- conv_bc: float32 [4, 2, 128], replicated, may hold values from -3 to 3
- conv_bc_b: float32 [2, 128], replicated, may hold values from -0.5 to 0.5
- dt_bias: float32 [48], P('tensor'), may hold values from -6.5 to -2.5
- a_log: float32 [48], P('tensor'), may hold values from 0 to 2.7
- d_skip: float32 [48], P('tensor'), may hold values from 0.5 to 1.5
- gain_norm: float32 [3072], P('tensor'), may hold values from 0.1 to 1.9
- w_out: bfloat16 [1536, 3072], P(('dp', 'seq'), 'tensor'), may hold values from -0.109375 to 0.109375
- cotangent: bfloat16 [4096, 4, 1536], P(('seq', 'tensor'), 'dp'), may hold values from -6 to 6
Outputs:
- block_output: bfloat16 [4096, 4, 1536], P(('seq', 'tensor'), 'dp')
- input_grad: bfloat16 [4096, 4, 1536], P(('seq', 'tensor'), 'dp')
- grad_gain_in: float32 [1536], replicated
- grad_w_zx: float32 [1536, 2, 3072], P(('dp', 'seq'), None, 'tensor')
- grad_w_bc: float32 [1536, 2, 128], P(('dp', 'seq'))
- grad_w_dt: float32 [1536, 48], P(('dp', 'seq'), 'tensor')
- grad_conv_x: float32 [4, 3072], P(None, 'tensor')
- grad_conv_x_b: float32 [3072], P('tensor')
- grad_conv_bc: float32 [4, 2, 128], replicated
- grad_conv_bc_b: float32 [2, 128], replicated
- grad_dt_bias: float32 [48], P('tensor')
- grad_a_log: float32 [48], P('tensor')
- grad_d_skip: float32 [48], P('tensor')
- grad_gain_norm: float32 [3072], P('tensor')
- grad_w_out: float32 [1536, 3072], P(('dp', 'seq'), 'tensor')
The draws below stay inside these ranges and needn't reach their ends.
All inputs are finite; a program needn't handle non-finite values.
Results may differ from the reference program's by a relative error of at most 0.012.
Values may be sent and summed in bfloat16 or wider, within the bound.
A program may use at most 320 MiB of HBM per device.

```python
import jax
import jax.numpy as jnp
from jax import lax

D = 1536
H = 48
N = 128
K = 4
L = 256
DI = 3072
SPAN = 1024
SEQLEN = 4096
SEQS = 4
N_SEQ = 4


def level_of(rng, shape, cuts, smallest, top_value):
    def one(position, parts):
        draws = jax.random.uniform(jax.random.fold_in(jax.random.fold_in(rng, 6), position), (parts,), jnp.float32, smallest / len(cuts), top_value / len(cuts))
        return jnp.repeat(jnp.exp(draws), shape[position] // parts).reshape((-1,) + (1,) * (len(shape) - position - 1))

    factor_of = one(*cuts[0])
    for cut in cuts[1:]:
        factor_of = factor_of * one(*cut)
    return factor_of


def normal_values(own_key, dims, spread, limit, split=(), held_as=jnp.bfloat16):
    array = spread * jax.random.normal(own_key, dims, jnp.float32)
    if split:
        array = array * level_of(own_key, dims, split, -0.22, 0.18)
    return jnp.clip(array, -limit, limit).astype(held_as)


def setup_inputs(seed: int = 0) -> dict:
    keys = jax.random.split(jax.random.key(seed), 16)
    block_input = normal_values(keys[0], (SEQLEN, SEQS, D), 1.0, 6.0, ((0, 16), (1, 2)))
    gain_in = jnp.clip(1.0 + 0.18 * jax.random.normal(keys[1], (D,), jnp.float32), 0.1, 1.9)
    w_zx = normal_values(keys[2], (D, 2, DI), D ** -0.5, 0.15625, ((0, 8), (2, 4)))
    w_bc = normal_values(keys[3], (D, 2, N), D ** -0.5, 0.15625, ((0, 8),))
    w_dt = normal_values(keys[4], (D, H), D ** -0.5, 0.15625, ((0, 8), (1, 4)))
    conv_x = normal_values(keys[5], (K, DI), K ** -0.5, 3.0, ((1, 4),), jnp.float32)
    conv_x_b = jnp.clip(jax.random.uniform(keys[6], (DI,), jnp.float32, -0.5, 0.5) * level_of(keys[6], (DI,), ((0, 4),), -0.4, 0.0), -0.5, 0.5)
    conv_bc = normal_values(keys[7], (K, 2, N), K ** -0.5, 3.0, (), jnp.float32)
    conv_bc_b = jnp.clip(jax.random.uniform(keys[8], (2, N), jnp.float32, -0.5, 0.5), -0.5, 0.5)
    dt_bias = jnp.clip(-6.5 + 4.0 * jax.random.uniform(keys[9], (H,), jnp.float32) ** level_of(keys[9], (H,), ((0, 4),), -0.2, 0.2), -6.5, -2.5)
    a_log = jnp.clip(2.7 * jax.random.uniform(keys[10], (H,), jnp.float32) ** level_of(keys[10], (H,), ((0, 4),), -0.2, 0.2), 0.0, 2.7)
    d_skip = jnp.clip(0.5 + 1.0 * jax.random.uniform(keys[11], (H,), jnp.float32) ** level_of(keys[11], (H,), ((0, 4),), -0.2, 0.2), 0.5, 1.5)
    gain_norm = jnp.clip(1.0 + 0.18 * jax.random.normal(keys[12], (DI,), jnp.float32), 0.1, 1.9)
    w_out = normal_values(keys[13], (D, DI), DI ** -0.5, 0.109375, ((0, 8), (1, 4)))
    cotangent = normal_values(keys[14], (SEQLEN, SEQS, D), 1.0, 6.0, ((0, 16), (1, 2)))
    return {"block_input": block_input, "gain_in": gain_in, "w_zx": w_zx, "w_bc": w_bc, "w_dt": w_dt, "conv_x": conv_x, "conv_x_b": conv_x_b, "conv_bc": conv_bc, "conv_bc_b": conv_bc_b, "dt_bias": dt_bias, "a_log": a_log, "d_skip": d_skip, "gain_norm": gain_norm, "w_out": w_out, "cotangent": cotangent}


epsilon = 1e-05
highest = lax.Precision.HIGHEST

def conv_acts(x_ext, bc_ext, dt_raw, conv_x, conv_x_b, conv_bc, conv_bc_b, dt_bias, a_log):
    span_len = dt_raw.shape[0]
    batch_size = dt_raw.shape[1]
    head_count = dt_raw.shape[2]
    tap_count = conv_x.shape[0]
    x_conv = conv_x_b + conv_x[0] * x_ext[0:span_len]
    bc_conv = conv_bc_b + conv_bc[0] * bc_ext[0:span_len]
    for k in range(1, tap_count):
        x_conv = x_conv + conv_x[k] * x_ext[k:k + span_len]
        bc_conv = bc_conv + conv_bc[k] * bc_ext[k:k + span_len]
    x_full = jax.nn.silu(x_conv)
    bc_full = jax.nn.silu(bc_conv)
    group_count = span_len // L
    head_dim = x_full.shape[2] // head_count
    state_size = bc_full.shape[3]
    x_act = x_full.reshape(group_count, L, batch_size, head_count, head_dim)
    b_rows = bc_full[:, :, 0].reshape(group_count, L, batch_size, state_size)
    c_rows = bc_full[:, :, 1].reshape(group_count, L, batch_size, state_size)
    time_step = jax.nn.softplus(dt_raw + dt_bias).reshape(group_count, L, batch_size, head_count)
    cum_decay = jnp.cumsum(time_step * -jnp.exp(a_log), axis=1)
    return (x_act, b_rows, c_rows, time_step, cum_decay)

def group_states(x_act, b_rows, time_step, cum_decay):
    last_decay = cum_decay[:, -1]
    weights = jnp.exp(last_decay[:, None] - cum_decay) * time_step
    weighted = weights[..., None] * x_act
    local_states = jnp.einsum('clbhp,clbn->cbhpn', weighted, b_rows, precision=highest)
    group_decay = jnp.exp(last_decay)
    running = jnp.zeros_like(local_states[0])
    entering = []
    for index in range(local_states.shape[0]):
        entering.append(running)
        running = group_decay[index][..., None, None] * running + local_states[index]
    return (jnp.stack(entering), running, jnp.exp(lax.optimization_barrier(jnp.sum(last_decay, axis=0))))

def group_output(x_act, b_rows, c_rows, time_step, cum_decay, d_skip, entering, state_in):
    scores = jnp.einsum('ctbn,csbn->ctsb', c_rows, b_rows, precision=highest)
    length = cum_decay.shape[1]
    causal = (jnp.arange(length)[:, None] >= jnp.arange(length)[None, :])[None, :, :, None, None]
    gaps = cum_decay[:, :, None] - cum_decay[:, None, :]
    lower = jnp.where(causal, jnp.exp(jnp.where(causal, gaps, 0.0)), 0.0)
    mixing = scores[..., None] * lower * time_step[:, None]
    intra = jnp.einsum('ctsbh,csbhp->ctbhp', mixing, x_act, precision=highest)
    last_decay = cum_decay[:, -1]
    before = jnp.exp(jnp.cumsum(last_decay, axis=0) - last_decay)
    states = entering + before[..., None, None] * state_in[None]
    inter = jnp.exp(cum_decay)[..., None] * jnp.einsum('ctbn,cbhpn->ctbhp', c_rows, states, precision=highest)
    total = intra + inter + d_skip[:, None] * x_act
    shape = x_act.shape
    return total.reshape(shape[0] * shape[1], shape[2], shape[3] * shape[4])

def mixer_norm(gate_in, x_pre, bc_pre, dt_raw, conv_x, conv_x_b, conv_bc, conv_bc_b, dt_bias, a_log, d_skip, gain_norm):
    tap_count = conv_x.shape[0]
    pad_x = jnp.concatenate([jnp.zeros((tap_count - 1,) + x_pre.shape[1:], x_pre.dtype), x_pre], 0)
    pad_bc = jnp.concatenate([jnp.zeros((tap_count - 1,) + bc_pre.shape[1:], bc_pre.dtype), bc_pre], 0)
    head_count = dt_raw.shape[2]
    state_in = jnp.zeros((dt_raw.shape[1], head_count, x_pre.shape[2] // head_count, bc_pre.shape[3]), x_pre.dtype)
    pieces = []
    for index in range(N_SEQ):
        low = index * SPAN
        acts = conv_acts(pad_x[low:low + SPAN + tap_count - 1], pad_bc[low:low + SPAN + tap_count - 1], dt_raw[low:low + SPAN], conv_x, conv_x_b, conv_bc, conv_bc_b, dt_bias, a_log)
        entering, local_state, decay = group_states(acts[0], acts[1], acts[3], acts[4])
        pieces.append(group_output(acts[0], acts[1], acts[2], acts[3], acts[4], d_skip, entering, state_in))
        state_in = decay[..., None, None] * state_in + local_state
    mixed = jnp.concatenate(pieces, 0)
    gated = mixed * jax.nn.silu(gate_in)
    inv_norm = lax.rsqrt(lax.optimization_barrier(jnp.mean(gated * gated, -1, keepdims=True)) + epsilon)
    return gated * inv_norm * gain_norm

def reference(block_input, gain_in, w_zx, w_bc, w_dt, conv_x, conv_x_b, conv_bc, conv_bc_b, dt_bias, a_log, d_skip, gain_norm, w_out, cotangent):
    width = block_input.shape[2]
    inner = gain_norm.shape[0]
    state_size = conv_bc.shape[2]
    zx_flat = w_zx.reshape(width, 2 * inner)
    bc_flat = w_bc.reshape(width, 2 * state_size)

    def one_sequence(totals, pair):
        seq_in, seq_cot = pair
        flat_in = seq_in.astype(jnp.float32)
        inv_in = lax.rsqrt(lax.optimization_barrier(jnp.mean(flat_in * flat_in, -1, keepdims=True)) + epsilon)
        base = flat_in * inv_in
        normed = (base * gain_in).astype(jnp.bfloat16)
        length = seq_in.shape[0]
        proj = jnp.dot(normed, zx_flat, preferred_element_type=jnp.float32)
        gate_in = proj[:, :inner][:, None]
        x_pre = proj[:, inner:][:, None]
        bc_pre = jnp.dot(normed, bc_flat, preferred_element_type=jnp.float32).reshape(length, 1, 2, state_size)
        dt_raw = jnp.dot(normed, w_dt, preferred_element_type=jnp.float32)[:, None]
        normed_out, pullback = jax.vjp(mixer_norm, gate_in, x_pre, bc_pre, dt_raw, conv_x, conv_x_b, conv_bc, conv_bc_b, dt_bias, a_log, d_skip, gain_norm)
        hidden = normed_out[:, 0].astype(jnp.bfloat16)
        branch = jnp.dot(hidden, w_out.T, preferred_element_type=jnp.float32)
        result = (flat_in + branch).astype(jnp.bfloat16)
        grad_hidden = jnp.dot(seq_cot, w_out, preferred_element_type=jnp.float32)
        grad_out_w = jnp.dot(seq_cot.T, hidden, preferred_element_type=jnp.float32)
        cot_mid = pullback(grad_hidden[:, None])
        cot_zx = jnp.concatenate([cot_mid[0][:, 0], cot_mid[1][:, 0]], -1).astype(jnp.bfloat16)
        cot_bc = cot_mid[2].reshape(length, 2 * state_size).astype(jnp.bfloat16)
        cot_dt = cot_mid[3][:, 0].astype(jnp.bfloat16)
        grad_normed = jnp.dot(cot_zx, zx_flat.T, preferred_element_type=jnp.float32) + jnp.dot(cot_bc, bc_flat.T, preferred_element_type=jnp.float32) + jnp.dot(cot_dt, w_dt.T, preferred_element_type=jnp.float32)
        scaled = grad_normed * gain_in
        grad_base = inv_in * (scaled - base * lax.optimization_barrier(jnp.mean(scaled * base, -1, keepdims=True)))
        grad_in = (seq_cot.astype(jnp.float32) + grad_base).astype(jnp.bfloat16)
        new_totals = (totals[0] + lax.optimization_barrier(jnp.sum(grad_normed * base, 0)), totals[1] + jnp.dot(normed.T, cot_zx, preferred_element_type=jnp.float32).reshape(width, 2, inner), totals[2] + jnp.dot(normed.T, cot_bc, preferred_element_type=jnp.float32).reshape(width, 2, state_size), totals[3] + jnp.dot(normed.T, cot_dt, preferred_element_type=jnp.float32), totals[4] + cot_mid[4], totals[5] + cot_mid[5], totals[6] + cot_mid[6], totals[7] + cot_mid[7], totals[8] + cot_mid[8], totals[9] + cot_mid[9], totals[10] + cot_mid[10], totals[11] + cot_mid[11], totals[12] + grad_out_w)
        return (new_totals, (result, grad_in))
    inits = (jnp.zeros(gain_in.shape, jnp.float32), jnp.zeros(w_zx.shape, jnp.float32), jnp.zeros(w_bc.shape, jnp.float32), jnp.zeros(w_dt.shape, jnp.float32), jnp.zeros(conv_x.shape, jnp.float32), jnp.zeros(conv_x_b.shape, jnp.float32), jnp.zeros(conv_bc.shape, jnp.float32), jnp.zeros(conv_bc_b.shape, jnp.float32), jnp.zeros(dt_bias.shape, jnp.float32), jnp.zeros(a_log.shape, jnp.float32), jnp.zeros(d_skip.shape, jnp.float32), jnp.zeros(gain_norm.shape, jnp.float32), jnp.zeros(w_out.shape, jnp.float32))
    sequences = (jnp.swapaxes(block_input, 0, 1), jnp.swapaxes(cotangent, 0, 1))
    totals, outputs = lax.scan(one_sequence, inits, sequences)
    return (jnp.swapaxes(outputs[0], 0, 1), jnp.swapaxes(outputs[1], 0, 1), totals[0], totals[1], totals[2], totals[3], totals[4], totals[5], totals[6], totals[7], totals[8], totals[9], totals[10], totals[11], totals[12])
```

```python
import functools

import jax
import jax.numpy as jnp
from jax import lax
from jax.experimental import pallas as pl
from jax.experimental.pallas import tpu as pltpu
from jax.sharding import PartitionSpec as P

L = 256
HD = 64
LANES = 128
EPS = 1e-05
F32 = jnp.float32
BF = jnp.bfloat16
MESH = pl.DeviceIdType.MESH
VMEM_LIMIT = 60 * 1024 * 1024
NEG = -1e30


def dot(a, b):
    return jnp.dot(a, b, preferred_element_type=F32)


def dot_nt(a, b):
    return lax.dot_general(a, b, (((1,), (1,)), ((), ())), preferred_element_type=F32)


def split(v):
    hi = v.astype(BF)
    return hi, (v - hi.astype(F32)).astype(BF)


def dot_split(mat, v):
    hi, lo = split(v)
    return dot(mat, hi) + dot(mat, lo)


def split_dot(v, mat):
    hi, lo = split(v)
    return dot(hi, mat) + dot(lo, mat)


def iota(shape, axis):
    return lax.broadcasted_iota(jnp.int32, shape, axis)


def pair_of(col, i, low):
    rows = col.shape[0]
    a = jnp.broadcast_to(col[:, 2 * i : 2 * i + 1], (rows, LANES))
    b = jnp.broadcast_to(col[:, 2 * i + 1 : 2 * i + 2], (rows, LANES))
    return jnp.where(low[:rows], a, b)


def segments(i):
    r, c = iota((LANES, LANES), 0), iota((LANES, LANES), 1)
    return jnp.where(c == 2 * i + jnp.where(r >= HD, 1, 0), 1.0, 0.0).astype(BF)


def sigmoid(v):
    return 1.0 / (1.0 + jnp.exp(-v))


def softplus(z):
    return jnp.maximum(z, 0.0) + jnp.log1p(jnp.exp(-jnp.abs(z)))


def acts_kernel(
    pairs,
    x_ref,
    bc_ref,
    dt_ref,
    halo_ref,
    cx_ref,
    cbc_ref,
    small_ref,
    xa_ref,
    dsx_ref,
    bca_ref,
    dsbc_ref,
    time_ref,
    cum_ref,
    state_ref,
    tot_ref,
    ext_x,
    ext_bc,
):
    j = pl.program_id(1)
    width = pairs * LANES

    @pl.when(j == 0)
    def _():
        ext_x[0:8, :] = halo_ref[0, :, 0:width]
        ext_bc[0:8, :] = halo_ref[0, :, width : width + 2 * LANES]
        state_ref[...] = jnp.zeros_like(state_ref)
        tot_ref[...] = jnp.zeros_like(tot_ref)

    ext_x[8 : 8 + L, :] = x_ref[0]
    ext_bc[8 : 8 + L, :] = bc_ref[0]
    low = iota((L, LANES), 1) < HD
    z = dt_ref[0] + small_ref[0:1, :]
    step = softplus(z)
    tri = jnp.where(iota((L, L), 0) >= iota((L, L), 1), 1.0, 0.0).astype(BF)
    rate = step * small_ref[1:2, :]
    r1 = rate.astype(BF)
    rest = rate - r1.astype(F32)
    r2 = rest.astype(BF)
    r3 = (rest - r2.astype(F32)).astype(BF)
    cum = dot(tri, r1) + dot(tri, r2) + dot(tri, r3)
    time_ref[0] = step
    cum_ref[0] = cum
    last = cum[L - 1 : L, :]
    tot_ref[0] = tot_ref[0] + jnp.broadcast_to(last, (8, LANES))
    decay = jnp.exp(last)
    weight = jnp.exp(last - cum) * step

    def act(ext, taps, at):
        v = taps[4:5, at] + taps[0:1, at] * ext[5 : 5 + L, at]
        for k in range(1, 4):
            v = v + taps[k : k + 1, at] * ext[5 + k : 5 + k + L, at]
        s = sigmoid(v)
        a = v * s
        return a, s * (1.0 + v * (1.0 - s))

    b_t = None
    for i in range(2):
        at = slice(i * LANES, (i + 1) * LANES)
        a, d = act(ext_bc, cbc_ref, at)
        bca_ref[0, :, at] = a
        dsbc_ref[0, :, at] = d.astype(BF)
        if i == 0:
            b_t = a.T.astype(BF)
    for i in range(pairs):
        at = slice(i * LANES, (i + 1) * LANES)
        a, d = act(ext_x, cx_ref, at)
        xa_ref[0, :, at] = a
        dsx_ref[0, :, at] = d.astype(BF)
        wx = (a * pair_of(weight, i, low)).astype(BF)
        state_ref[0, :, at] = state_ref[0, :, at] * pair_of(decay, i, low) + dot(b_t, wx)
    ext_x[0:8, :] = ext_x[L : L + 8, :]
    ext_bc[0:8, :] = ext_bc[L : L + 8, :]


def forward_kernel(
    pairs,
    x_ref,
    bc_ref,
    time_ref,
    cum_ref,
    gate_ref,
    gh_ref,
    in_ref,
    chan_ref,
    mixed_ref,
    ent_ref,
    aft_ref,
    stat_ref,
    state,
):
    j = pl.program_id(1)

    @pl.when(j == 0)
    def _():
        state[...] = in_ref[0]

    low = iota((L, LANES), 1) < HD
    b_t, b_lo = split(bc_ref[0, :, 0:LANES].T)
    c, c_lo = split(bc_ref[0, :, LANES : 2 * LANES])
    scores = dot(c, b_t) + (dot(c, b_lo) + dot(c_lo, b_t))
    step, cum = time_ref[0], cum_ref[0]
    cum_t = cum.T
    last = cum[L - 1 : L, :]
    decay = jnp.exp(last)
    grow = jnp.exp(cum)
    weight = jnp.exp(last - cum) * step
    half = L // 2
    mask = jnp.where(iota((half, half), 0) >= iota((half, half), 1), 0.0, NEG)
    squares = jnp.zeros((L, LANES), F32)
    inner = jnp.zeros((L, LANES), F32)
    for i in range(pairs):
        at = slice(i * LANES, (i + 1) * LANES)
        x = x_ref[0, :, at]
        xdt = x * pair_of(step, i, low)
        xdt_b, xdt_lo = split(xdt)
        old = state[:, at]
        old_b, old_lo = split(old)
        ent_ref[0, 0, :, at] = old_b
        y = pair_of(grow, i, low) * (dot(c, old_b) + dot(c, old_lo))
        new = old * pair_of(decay, i, low) + dot_split(b_t, x * pair_of(weight, i, low))
        state[:, at] = new
        aft_ref[0, 0, :, at] = new
        tops = jnp.zeros((half, LANES), F32)
        bots = jnp.zeros((half, LANES), F32)
        zero = jnp.zeros_like(xdt_b)
        for s in range(2):
            h = 2 * i + s
            xm = jnp.where(low, xdt_b, zero) if s == 0 else jnp.where(low, zero, xdt_b)
            xl = jnp.where(low, xdt_lo, zero) if s == 0 else jnp.where(low, zero, xdt_lo)
            top = jnp.exp(cum[:half, h : h + 1] - cum_t[h : h + 1, :half] + mask)
            mix = (top * scores[:half, :half]).astype(BF)
            tops = tops + (dot(mix, xm[:half]) + dot(mix, xl[:half]))
            left = jnp.exp(cum[half:, h : h + 1] - cum_t[h : h + 1, :half])
            right = jnp.exp(cum[half:, h : h + 1] - cum_t[h : h + 1, half:] + mask)
            mix = jnp.concatenate(
                [
                    (left * scores[half:, :half]).astype(BF),
                    (right * scores[half:, half:]).astype(BF),
                ],
                axis=1,
            )
            bots = bots + (dot(mix, xm) + dot(mix, xl))
        y = y + jnp.concatenate([tops, bots], axis=0)
        mixed = y + chan_ref[0:1, at] * x
        mixed_ref[0, :, at] = mixed
        gate = gate_ref[0, :, at]
        gated = mixed * (gate * sigmoid(gate))
        squares = squares + gated * gated
        inner = inner + gated * (gh_ref[0, :, at] * chan_ref[1:2, at])
    lane = iota((L, LANES), 1)
    both = jnp.where(
        lane == 0,
        jnp.sum(squares, axis=1, keepdims=True),
        jnp.where(lane == 1, jnp.sum(inner, axis=1, keepdims=True), 0.0),
    )
    stat_ref[0] = both.T[0:2, :]


def gating_kernel(
    pairs,
    total,
    x_ref,
    bc_ref,
    cum_ref,
    gate_ref,
    gh_ref,
    mixed_ref,
    stat_ref,
    chan_ref,
    grad_ref,
    cgate_ref,
    hidden_ref,
    ds_ref,
    sums_ref,
    before,
):
    n, j = pl.program_id(0), pl.program_id(1)

    @pl.when(j == 0)
    def _():
        before[...] = jnp.zeros_like(before)
        ds_ref[...] = jnp.zeros_like(ds_ref)

    @pl.when((j == 0) & (n == 0))
    def _():
        sums_ref[...] = jnp.zeros_like(sums_ref)

    low = iota((L, LANES), 1) < HD
    rows = iota((LANES, L), 0)
    stat = jnp.where(
        rows == 0,
        jnp.broadcast_to(stat_ref[0, 0:1, :], (LANES, L)),
        jnp.broadcast_to(stat_ref[0, 1:2, :], (LANES, L)),
    ).T
    inv = lax.rsqrt(stat[:, 0:1] * (1.0 / total) + EPS)
    back = inv * inv * inv * (stat[:, 1:2] * (1.0 / total))
    inv = jnp.broadcast_to(inv, (L, LANES))
    back = jnp.broadcast_to(back, (L, LANES))
    cum = cum_ref[0]
    grow = jnp.exp(cum + before[0:1, :])
    before[...] = before[...] + jnp.broadcast_to(cum[L - 1 : L, :], before.shape)
    c_t = bc_ref[0, :, LANES : 2 * LANES].T.astype(BF)
    for i in range(pairs):
        at = slice(i * LANES, (i + 1) * LANES)
        x = x_ref[0, :, at]
        gate = gate_ref[0, :, at]
        mixed = mixed_ref[0, :, at]
        gh = gh_ref[0, :, at]
        gain = chan_ref[1:2, at]
        sig = sigmoid(gate)
        act = gate * sig
        gated = mixed * act
        normal = gated * inv
        hidden_ref[0, :, at] = (normal * gain).astype(BF)
        grad_gated = inv * (gh * gain) - gated * back
        grad = grad_gated * act
        grad_ref[0, :, at] = grad
        cgate_ref[0, :, at] = (grad_gated * mixed * sig * (1.0 + gate * (1.0 - sig))).astype(BF)
        ds_ref[0, :, at] = ds_ref[0, :, at] + dot(
            c_t, (grad * pair_of(grow, i, low)).astype(BF)
        )
        sums_ref[0:1, at] = sums_ref[0:1, at] + jnp.sum(gh * normal, axis=0, keepdims=True)
        sums_ref[1:2, at] = sums_ref[1:2, at] + jnp.sum(grad * x, axis=0, keepdims=True)


def backward_kernel(
    pairs,
    grad_ref,
    cgate_ref,
    x_ref,
    dsx_ref,
    bc_ref,
    dsbc_ref,
    time_ref,
    cum_ref,
    ent_ref,
    aft_ref,
    mixed_ref,
    px_ref,
    pbc_ref,
    pdt_ref,
    halo_ref,
    carried_ref,
    chan_ref,
    cx_ref,
    cbc_ref,
    small_ref,
    cot_ref,
    tail_ref,
    sx_ref,
    sbc_ref,
    sdt_ref,
    state,
    ext_x,
    ext_bc,
):
    n, g = pl.program_id(0), pl.program_id(1)
    final = pl.num_programs(1) - 1
    width = pairs * LANES

    @pl.when(g == 0)
    def _():
        state[...] = carried_ref[0]
        ext_x[L : L + 8, :] = jnp.zeros((8, width), F32)
        ext_bc[L : L + 8, :] = jnp.zeros((8, 2 * LANES), F32)

    @pl.when((g == 0) & (n == 0))
    def _():
        sx_ref[...] = jnp.zeros_like(sx_ref)
        sbc_ref[...] = jnp.zeros_like(sbc_ref)
        sdt_ref[...] = jnp.zeros_like(sdt_ref)

    low = iota((L, LANES), 1) < HD
    b, b_lo = split(bc_ref[0, :, 0:LANES])
    c_full = bc_ref[0, :, LANES : 2 * LANES]
    c = c_full.astype(BF)
    c_t, c_lo = split(c_full.T)
    scores_t = dot(b, c_t) + (dot(b, c_lo) + dot(b_lo, c_t))
    step, cum = time_ref[0], cum_ref[0]
    cum_t = cum.T
    last = cum[L - 1 : L, :]
    decay = jnp.exp(last)
    grow = jnp.exp(cum)
    fade = jnp.exp(last - cum)
    half = L // 2
    mask = jnp.where(iota((half, half), 1) >= iota((half, half), 0), 0.0, NEG)
    grad_b = jnp.zeros((L, LANES), F32)
    grad_c = jnp.zeros((L, LANES), F32)
    ds_a = jnp.zeros((half, half), F32)
    ds_b = jnp.zeros((half, half), F32)
    ds_d = jnp.zeros((half, half), F32)
    dcum = jnp.zeros((L, LANES), F32)
    cols = jnp.zeros((L, LANES), F32)
    dlast = jnp.zeros((8, LANES), F32)

    for i in range(pairs):
        at = slice(i * LANES, (i + 1) * LANES)
        seg = segments(i)
        x = x_ref[0, :, at]
        dt_e = pair_of(step, i, low)
        fade_e = pair_of(fade, i, low)
        xdt = x * dt_e
        xdt_b = xdt.astype(BF)
        gm = grad_ref[0, :, at]
        gm_b, gm_lo = split(gm)
        grow_g, grow_lo = split(gm * pair_of(grow, i, low))
        ds_old = state[:, at]
        ds_old_b, ds_old_lo = split(ds_old)
        dxdt = fade_e * (dot(b, ds_old_b) + dot(b, ds_old_lo))
        grad_b = grad_b + dot_nt((xdt * fade_e).astype(BF), ds_old_b)
        grad_c = grad_c + dot_nt(grow_g, ent_ref[0, 0, :, at])
        lasts = jnp.sum(aft_ref[0, 0, :, at] * ds_old, axis=0, keepdims=True)
        dlast = dlast + split_dot(jnp.broadcast_to(lasts, (8, LANES)), seg)
        state[:, at] = ds_old * pair_of(decay, i, low) + (dot(c_t, grow_g) + dot(c_t, grow_lo))
        zero = jnp.zeros_like(xdt_b)
        tops = jnp.zeros((half, LANES), F32)
        bots = jnp.zeros((half, LANES), F32)
        for s in range(2):
            h = 2 * i + s
            xm = jnp.where(low, xdt_b, zero) if s == 0 else jnp.where(low, zero, xdt_b)
            gs = jnp.where(low, gm_b, zero) if s == 0 else jnp.where(low, zero, gm_b)
            gl = jnp.where(low, gm_lo, zero) if s == 0 else jnp.where(low, zero, gm_lo)
            row, col = cum_t[h : h + 1, :], cum[:, h : h + 1]
            low_a = jnp.exp(row[:, :half] - col[:half] + mask)
            low_b = jnp.exp(row[:, half:] - col[:half])
            low_d = jnp.exp(row[:, half:] - col[half:] + mask)
            dm_top = dot_nt(xm[:half], gm_b)
            dm_bot = dot_nt(xm[half:], gm_b[half:])
            ds_a = ds_a + dm_top[:, :half] * low_a
            ds_b = ds_b + dm_top[:, half:] * low_b
            ds_d = ds_d + dm_bot * low_d
            mix = jnp.concatenate(
                [
                    (low_a * scores_t[:half, :half]).astype(BF),
                    (low_b * scores_t[:half, half:]).astype(BF),
                ],
                axis=1,
            )
            tops = tops + (dot(mix, gs) + dot(mix, gl))
            mix = (low_d * scores_t[half:, half:]).astype(BF)
            bots = bots + (dot(mix, gs[half:]) + dot(mix, gl[half:]))
        dxdt = dxdt + jnp.concatenate([tops, bots], axis=0)
        skip = chan_ref[0:1, at]
        dcum = dcum + split_dot(gm * (mixed_ref[0, :, at] - skip * x), seg)
        cols = cols + split_dot(xdt * dxdt, seg)
        gx = (dt_e * dxdt + skip * gm) * dsx_ref[0, :, at].astype(F32)
        ext_x[0:L, at] = gx
        px = px_ref[0, :, at]
        cot = cx_ref[3:4, at] * gx
        sx_ref[3:4, at] = sx_ref[3:4, at] + jnp.sum(px * gx, axis=0, keepdims=True)
        sx_ref[4:5, at] = sx_ref[4:5, at] + jnp.sum(gx, axis=0, keepdims=True)
        for k in range(3):
            moved = ext_x[3 - k : 3 - k + L, at]
            cot = cot + cx_ref[k : k + 1, at] * moved
            sx_ref[k : k + 1, at] = sx_ref[k : k + 1, at] + jnp.sum(
                px * moved, axis=0, keepdims=True
            )
        cot_ref[0, :, at] = cgate_ref[0, :, at]
        cot_ref[0, :, width + i * LANES : width + (i + 1) * LANES] = cot.astype(BF)

    zero = jnp.zeros((half, half), F32)
    ds_t = jnp.concatenate(
        [jnp.concatenate([ds_a, ds_b], axis=1), jnp.concatenate([zero, ds_d], axis=1)], axis=0
    )
    grad_b = grad_b + dot(ds_t.astype(BF), c)
    grad_c = grad_c + dot(ds_t.T.astype(BF), b)
    for i, part in ((0, grad_b), (1, grad_c)):
        at = slice(i * LANES, (i + 1) * LANES)
        gb = part * dsbc_ref[0, :, at].astype(F32)
        ext_bc[0:L, at] = gb
        pb = pbc_ref[0, :, at]
        cot = cbc_ref[3:4, at] * gb
        sbc_ref[3:4, at] = sbc_ref[3:4, at] + jnp.sum(pb * gb, axis=0, keepdims=True)
        sbc_ref[4:5, at] = sbc_ref[4:5, at] + jnp.sum(gb, axis=0, keepdims=True)
        for k in range(3):
            moved = ext_bc[3 - k : 3 - k + L, at]
            cot = cot + cbc_ref[k : k + 1, at] * moved
            sbc_ref[k : k + 1, at] = sbc_ref[k : k + 1, at] + jnp.sum(
                pb * moved, axis=0, keepdims=True
            )
        cot_ref[0, :, 2 * width + i * LANES : 2 * width + (i + 1) * LANES] = cot.astype(BF)

    upper = jnp.where(iota((L, L), 1) >= iota((L, L), 0), 1.0, 0.0).astype(BF)
    drate = dot_split(upper, dcum - cols) + dlast[0:1, :]
    z = pdt_ref[0] + small_ref[0:1, :]
    sig = sigmoid(z)
    ratio = jnp.where(z < -15.0, 1.0, sig / jnp.where(z < -15.0, 1.0, step))
    dz = cols * ratio + drate * small_ref[1:2, :] * sig
    cot_ref[0, :, 2 * width + 2 * LANES : 2 * width + 3 * LANES] = dz.astype(BF)
    sdt_ref[0:1, :] = sdt_ref[0:1, :] + jnp.sum(dz, axis=0, keepdims=True)
    sdt_ref[1:2, :] = sdt_ref[1:2, :] + jnp.sum(
        drate * step * small_ref[1:2, :], axis=0, keepdims=True
    )

    @pl.when(g == final)
    def _():
        for ext, taps, sums, first, wide in (
            (ext_x, cx_ref, sx_ref, 0, width),
            (ext_bc, cbc_ref, sbc_ref, width, 2 * LANES),
        ):
            both = jnp.concatenate([jnp.zeros((8, wide), F32), ext[0:8, :]], axis=0)
            before = halo_ref[0, :, first : first + wide]
            total = jnp.zeros((8, wide), F32)
            for k in range(3):
                moved = both[3 - k : 11 - k, :]
                total = total + taps[k : k + 1, :] * moved
                sums[k : k + 1, :] = sums[k : k + 1, :] + jnp.sum(
                    before * moved, axis=0, keepdims=True
                )
            tail_ref[0, :, first : first + wide] = total
        tail_ref[0, :, width + 2 * LANES :] = jnp.zeros((8, LANES), F32)

    ext_x[L : L + 8, :] = ext_x[0:8, :]
    ext_bc[L : L + 8, :] = ext_bc[0:8, :]


def tensor_peers():
    me = lax.axis_index("tensor")
    chip, core = me // 2, lax.rem(me, 2)
    partner = chip * 2 + (1 - core)
    across = (1 - chip) * 2 + core
    return me, chip, core, partner, across


def greet(partner, across):
    barrier = pltpu.get_barrier_semaphore()
    for peer in (partner, across):
        pl.semaphore_signal(barrier, inc=1, device_id={"tensor": peer}, device_id_type=MESH)
    pl.semaphore_wait(barrier, 2)


def gather_kernel(cuts, count, *refs):
    ins, outs = refs[:count], refs[count : 2 * count]
    own_sem, near_s, near_r, far_s, far_r, pass_s, pass_r = refs[2 * count :]
    me, chip, core, partner, across = tensor_peers()
    greet(partner, across)
    batch, rows = ins[0].shape[0], ins[0].shape[1]
    piece = rows // cuts

    def remote(src, dst, send, recv, peer):
        return pltpu.make_async_remote_copy(
            src_ref=src,
            dst_ref=dst,
            send_sem=send,
            recv_sem=recv,
            device_id={"tensor": peer},
            device_id_type=MESH,
        )

    todo = []
    at = 0
    for a in range(count):
        for n in range(batch):
            for cut in range(cuts):
                mine = pl.ds(pl.multiple_of(me * rows + cut * piece, piece), piece)
                theirs = pl.ds(pl.multiple_of(across * rows + cut * piece, piece), piece)
                src = ins[a].at[n, cut * piece : (cut + 1) * piece, :]
                far = remote(src, outs[a].at[n, mine, :], far_s.at[at], far_r.at[at], across)
                near = remote(src, outs[a].at[n, mine, :], near_s.at[at], near_r.at[at], partner)
                own = pltpu.make_async_copy(src, outs[a].at[n, mine, :], own_sem.at[at])
                here = outs[a].at[n, theirs, :]
                onward = remote(here, here, pass_s.at[at], pass_r.at[at], partner)
                todo.append((far, near, own, onward))
                at += 1
    for far, near, own, onward in todo:
        far.start()
    for far, near, own, onward in todo:
        near.start()
        own.start()
    for far, near, own, onward in todo:
        far.wait_recv()
        onward.start()
    for far, near, own, onward in todo:
        far.wait_send()
        near.wait()
        own.wait()
        onward.wait()


def gather_tokens(*arrays):
    size = lax.axis_size("tensor")
    if size != 4:
        return [lax.all_gather(a, "tensor", axis=1, tiled=True) for a in arrays]
    batch, rows, width = arrays[0].shape
    count, cuts = len(arrays), 2
    sems = count * batch * cuts
    out = jax.ShapeDtypeStruct((batch, size * rows, width), arrays[0].dtype)
    return pl.pallas_call(
        functools.partial(gather_kernel, cuts, count),
        out_shape=[out] * count,
        in_specs=[pl.BlockSpec(memory_space=pltpu.VMEM)] * count,
        out_specs=[pl.BlockSpec(memory_space=pl.ANY)] * count,
        scratch_shapes=[pltpu.SemaphoreType.DMA((sems,))] * 7,
        compiler_params=pltpu.CompilerParams(
            collective_id=0, has_side_effects=True, vmem_limit_bytes=16 * 1024 * 1024
        ),
        name="gather_tokens",
    )(*arrays)


def scatter_kernel(cuts, in_ref, out_ref, near_buf, far_buf, sum_buf, near_s, near_r, far_s, far_r):
    me, chip, core, partner, across = tensor_peers()
    greet(partner, across)
    batch, rows = out_ref.shape[0], out_ref.shape[1]
    piece = rows // cuts

    def rows_of(owner, cut):
        return pl.ds(pl.multiple_of(owner * rows + cut * piece, piece), piece)

    def remote(src, dst, send, recv, peer):
        return pltpu.make_async_remote_copy(
            src_ref=src,
            dst_ref=dst,
            send_sem=send,
            recv_sem=recv,
            device_id={"tensor": peer},
            device_id_type=MESH,
        )

    near = {}
    for step, target in ((0, (1 - chip) * 2 + (1 - core)), (1, chip * 2 + (1 - core))):
        for n in range(batch):
            for cut in range(cuts):
                at = (step * batch + n) * cuts + cut
                near[step, n, cut] = remote(
                    in_ref.at[n, rows_of(target, cut), :],
                    near_buf.at[at],
                    near_s.at[at],
                    near_r.at[at],
                    partner,
                )
                near[step, n, cut].start()
    far = {}
    for n in range(batch):
        for cut in range(cuts):
            at = n * cuts + cut
            near[0, n, cut].wait_recv()
            sum_buf[at] = (
                in_ref[n, rows_of(across, cut), :].astype(F32) + near_buf[at].astype(F32)
            ).astype(BF)
            far[n, cut] = remote(
                sum_buf.at[at], far_buf.at[at], far_s.at[at], far_r.at[at], across
            )
            far[n, cut].start()
    for n in range(batch):
        for cut in range(cuts):
            at = n * cuts + cut
            near[1, n, cut].wait_recv()
            far[n, cut].wait_recv()
            out_ref[n, cut * piece : (cut + 1) * piece, :] = (
                in_ref[n, rows_of(me, cut), :].astype(F32)
                + near_buf[batch * cuts + at].astype(F32)
                + far_buf[at].astype(F32)
            )
    for key in near:
        near[key].wait_send()
    for key in far:
        far[key].wait_send()


def scatter_tokens(part, ident):
    size = lax.axis_size("tensor")
    if size != 4:
        return lax.psum_scatter(part, "tensor", scatter_dimension=1, tiled=True).astype(F32)
    batch, tokens, width = part.shape
    rows, cuts = tokens // size, 2
    piece = rows // cuts
    return pl.pallas_call(
        functools.partial(scatter_kernel, cuts),
        out_shape=jax.ShapeDtypeStruct((batch, rows, width), F32),
        in_specs=[pl.BlockSpec(memory_space=pltpu.VMEM)],
        out_specs=pl.BlockSpec(memory_space=pltpu.VMEM),
        scratch_shapes=[
            pltpu.VMEM((2 * batch * cuts, piece, width), BF),
            pltpu.VMEM((batch * cuts, piece, width), BF),
            pltpu.VMEM((batch * cuts, piece, width), BF),
            pltpu.SemaphoreType.DMA((2 * batch * cuts,)),
            pltpu.SemaphoreType.DMA((2 * batch * cuts,)),
            pltpu.SemaphoreType.DMA((batch * cuts,)),
            pltpu.SemaphoreType.DMA((batch * cuts,)),
        ],
        compiler_params=pltpu.CompilerParams(
            collective_id=ident, has_side_effects=True, vmem_limit_bytes=40 * 1024 * 1024
        ),
        name="scatter_tokens",
    )(part)


def chain_kernel(by, cuts, own_ref, tot_ref, out_ref, in_buf, send_buf, send_sem, recv_sem):
    me, size = lax.axis_index("seq"), lax.axis_size("seq")
    ahead, behind = me + by, me - by
    has_next = (ahead >= 0) & (ahead < size)
    has_prev = (behind >= 0) & (behind < size)
    barrier = pltpu.get_barrier_semaphore()

    @pl.when(has_next)
    def _():
        pl.semaphore_signal(barrier, inc=1, device_id={"seq": ahead}, device_id_type=MESH)

    @pl.when(has_prev)
    def _():
        pl.semaphore_signal(barrier, inc=1, device_id={"seq": behind}, device_id_type=MESH)

    pl.semaphore_wait(barrier, has_next.astype(jnp.int32) + has_prev.astype(jnp.int32))

    batch, rows = own_ref.shape[0], own_ref.shape[1] // cuts
    copies = []
    for n in range(batch):
        decay = jnp.exp(tot_ref[n, 0:1, :])
        for cut in range(cuts):
            at = n * cuts + cut
            here = slice(cut * rows, (cut + 1) * rows)
            copy = pltpu.make_async_remote_copy(
                src_ref=send_buf.at[at],
                dst_ref=in_buf.at[at],
                send_sem=send_sem.at[at],
                recv_sem=recv_sem.at[at],
                device_id={"seq": ahead},
                device_id_type=MESH,
            )
            copies.append(copy)

            @pl.when(has_prev)
            def _():
                copy.wait_recv()
                out_ref[n, here, :] = in_buf[at].astype(F32)

            @pl.when(jnp.logical_not(has_prev))
            def _():
                out_ref[n, here, :] = jnp.zeros((rows, out_ref.shape[2]), F32)

            @pl.when(has_next)
            def _():
                send_buf[at] = (out_ref[n, here, :] * decay + own_ref[n, here, :]).astype(BF)
                copy.start()

    @pl.when(has_next)
    def _():
        for copy in copies:
            copy.wait_send()


def chain(own, tot, by, ident):
    batch, rows, width = own.shape
    cuts = 4
    return pl.pallas_call(
        functools.partial(chain_kernel, by, cuts),
        out_shape=jax.ShapeDtypeStruct(own.shape, F32),
        in_specs=[pl.BlockSpec(memory_space=pltpu.VMEM)] * 2,
        out_specs=pl.BlockSpec(memory_space=pltpu.VMEM),
        scratch_shapes=[
            pltpu.VMEM((batch * cuts, rows // cuts, width), BF),
            pltpu.VMEM((batch * cuts, rows // cuts, width), BF),
            pltpu.SemaphoreType.DMA((batch * cuts,)),
            pltpu.SemaphoreType.DMA((batch * cuts,)),
        ],
        compiler_params=pltpu.CompilerParams(collective_id=ident, has_side_effects=True),
        name="chain",
    )(own, tot)


def sum_kernel(phases, in_ref, out_ref, *scratch):
    count = len(phases)
    bufs, sends, recvs = scratch[:count], scratch[count : 2 * count], scratch[2 * count :]
    barrier = pltpu.get_barrier_semaphore()
    greeted = 0
    for axis, _ in phases:
        me, size = lax.axis_index(axis), lax.axis_size(axis)
        for d in range(1, size):
            peer = lax.rem(me + d, size)
            pl.semaphore_signal(barrier, inc=1, device_id={axis: peer}, device_id_type=MESH)
            greeted += 1
    pl.semaphore_wait(barrier, greeted)
    out_ref[...] = in_ref[...]
    for p, (axis, first) in enumerate(phases):
        me, size = lax.axis_index(axis), lax.axis_size(axis)
        rows = in_ref.shape[0] - first
        bufs[p][pl.ds(me, 1)] = out_ref[first:, :].reshape(1, rows, LANES)
        copies = []
        for d in range(1, size):
            copies.append(
                pltpu.make_async_remote_copy(
                    src_ref=(in_ref if p == 0 else out_ref).at[pl.ds(first, rows), :],
                    dst_ref=bufs[p].at[me],
                    send_sem=sends[p].at[d - 1],
                    recv_sem=recvs[p].at[d - 1],
                    device_id={axis: lax.rem(me + d, size)},
                    device_id_type=MESH,
                )
            )
            copies[-1].start()
        for copy in copies:
            copy.wait()
        total = bufs[p][0]
        for r in range(1, size):
            total = total + bufs[p][r]
        out_ref[first:, :] = total


def small_sum(value, phases, ident):
    rows = value.shape[0]
    sizes = [lax.axis_size(axis) for axis, _ in phases]
    scratch = [pltpu.VMEM((n, rows - first, LANES), F32) for n, (_, first) in zip(sizes, phases)]
    scratch += [pltpu.SemaphoreType.DMA((max(n - 1, 1),)) for n in sizes] * 2
    return pl.pallas_call(
        functools.partial(sum_kernel, phases),
        out_shape=jax.ShapeDtypeStruct(value.shape, F32),
        in_specs=[pl.BlockSpec(memory_space=pltpu.VMEM)],
        out_specs=pl.BlockSpec(memory_space=pltpu.VMEM),
        scratch_shapes=scratch,
        compiler_params=pltpu.CompilerParams(collective_id=ident, has_side_effects=True),
        name="small_sum",
    )(value)


def rows_of_lanes(flat, unit=8 * LANES):
    short = -flat.shape[0] % unit
    return jnp.pad(flat, (0, short)).reshape(-1, LANES)


def shifted(value, by):
    peers = lax.axis_size("seq")
    pairs = [(i, i + by) for i in range(peers) if 0 <= i + by < peers]
    return lax.ppermute(value, "seq", pairs)


def pad_last(value, to):
    short = to - value.shape[-1]
    if short == 0:
        return value
    return jnp.pad(value, [(0, 0)] * (value.ndim - 1) + [(0, short)])


def token_spec(width, col=0, flip=None):
    if flip is None:
        return pl.BlockSpec((1, L, width), lambda n, j: (n, j, col))
    return pl.BlockSpec((1, L, width), lambda n, j: (n, flip - 1 - j, col))


def span_spec(shape):
    return pl.BlockSpec((1,) + shape, lambda n, j: (n,) + (0,) * len(shape))


def whole_spec(shape):
    return pl.BlockSpec(shape, lambda n, j: (0,) * len(shape))


def shards(
    block_input,
    gain_in,
    w_zx,
    w_bc,
    w_dt,
    conv_x,
    conv_x_b,
    conv_bc,
    conv_bc_b,
    dt_bias,
    a_log,
    d_skip,
    gain_norm,
    w_out,
    cotangent,
):
    rows_dev, batch, model = block_input.shape
    tensor_count = lax.axis_size("tensor")
    span = rows_dev * tensor_count
    groups = span // L
    heads = dt_bias.shape[0]
    inner = gain_norm.shape[0]
    inner_total = inner * tensor_count
    state_n = conv_bc.shape[2]
    pairs = (heads + 1) // 2
    width = pairs * LANES
    tails = width + 3 * LANES
    wide = width + tails
    rows_w = w_out.shape[0]
    pspace = ("dp", "seq")

    mine_in = jnp.concatenate(
        [
            pad_last(w_zx[:, 0], width),
            pad_last(w_zx[:, 1], width),
            w_bc.reshape(rows_w, 2 * state_n),
            pad_last(w_dt, LANES),
        ],
        axis=1,
    )
    mine_o = pad_last(w_out, width)
    full_in = lax.all_gather(mine_in, pspace, axis=0, tiled=True)
    full_in, mine_o = lax.optimization_barrier((full_in, mine_o))
    full_o = lax.all_gather(mine_o, pspace, axis=0, tiled=True)

    flat_in = jnp.swapaxes(block_input, 0, 1).astype(F32)
    cot_rows = jnp.swapaxes(cotangent, 0, 1)
    inv_in = lax.rsqrt(jnp.mean(flat_in * flat_in, -1, keepdims=True) + EPS)
    base = flat_in * inv_in
    normed_rows = (base * gain_in).astype(BF)
    normed, cots = gather_tokens(normed_rows, cot_rows)
    halo_rows = shifted(normed[:, span - 8 :], 1)

    taps_x = pad_last(jnp.concatenate([conv_x, conv_x_b[None], jnp.zeros((3, inner), F32)], 0), width)
    taps_bc = jnp.concatenate(
        [
            conv_bc.reshape(4, 2 * state_n),
            conv_bc_b.reshape(1, 2 * state_n),
            jnp.zeros((3, 2 * state_n), F32),
        ],
        0,
    )
    small = pad_last(jnp.stack([dt_bias, -jnp.exp(a_log)] + [jnp.zeros_like(a_log)] * 6), LANES)
    chan = pad_last(
        jnp.stack([jnp.repeat(d_skip, HD), gain_norm] + [jnp.zeros_like(gain_norm)] * 6), width
    )

    pre = jnp.einsum("btd,dk->btk", normed, full_in, preferred_element_type=F32)
    halo = jnp.einsum("btd,dk->btk", halo_rows, full_in[:, width:], preferred_element_type=F32)
    grad_hidden = jnp.einsum("btd,dk->btk", cots, full_o, preferred_element_type=F32)

    params = pltpu.CompilerParams(
        dimension_semantics=("arbitrary", "arbitrary"), vmem_limit_bytes=VMEM_LIMIT
    )
    grid = (batch, groups)
    at_bc, at_dt = pairs, 2 * pairs + 2
    sds = jax.ShapeDtypeStruct
    x_act, ds_x, bc_act, ds_bc, step, cum, local_state, tot = pl.pallas_call(
        functools.partial(acts_kernel, pairs),
        grid=grid,
        out_shape=[
            sds((batch, span, width), F32),
            sds((batch, span, width), BF),
            sds((batch, span, 2 * LANES), F32),
            sds((batch, span, 2 * LANES), BF),
            sds((batch, span, LANES), F32),
            sds((batch, span, LANES), F32),
            sds((batch, LANES, width), F32),
            sds((batch, 8, LANES), F32),
        ],
        in_specs=[
            token_spec(width, 1),
            token_spec(2 * LANES, at_bc),
            token_spec(LANES, at_dt),
            span_spec((8, tails)),
            whole_spec((8, width)),
            whole_spec((8, 2 * LANES)),
            whole_spec((8, LANES)),
        ],
        out_specs=[
            token_spec(width),
            token_spec(width),
            token_spec(2 * LANES),
            token_spec(2 * LANES),
            token_spec(LANES),
            token_spec(LANES),
            span_spec((LANES, width)),
            span_spec((8, LANES)),
        ],
        scratch_shapes=[pltpu.VMEM((L + 8, width), F32), pltpu.VMEM((L + 8, 2 * LANES), F32)],
        compiler_params=params,
        name="acts",
    )(pre, pre, pre, halo, taps_x, taps_bc, small)

    tot_wide = jnp.repeat(tot[:, :, : 2 * pairs], HD, axis=-1)
    state_in = chain(local_state, tot_wide, 1, 3)

    mixed, ent, aft, stats = pl.pallas_call(
        functools.partial(forward_kernel, pairs),
        grid=grid,
        out_shape=[
            sds((batch, span, width), F32),
            sds((batch, groups, LANES, width), BF),
            sds((batch, groups, LANES, width), F32),
            sds((batch, 2, span), F32),
        ],
        in_specs=[
            token_spec(width),
            token_spec(2 * LANES),
            token_spec(LANES),
            token_spec(LANES),
            token_spec(width),
            token_spec(width),
            span_spec((LANES, width)),
            whole_spec((8, width)),
        ],
        out_specs=[
            token_spec(width),
            pl.BlockSpec((1, 1, LANES, width), lambda n, j: (n, j, 0, 0)),
            pl.BlockSpec((1, 1, LANES, width), lambda n, j: (n, j, 0, 0)),
            pl.BlockSpec((1, 2, L), lambda n, j: (n, 0, j)),
        ],
        scratch_shapes=[pltpu.VMEM((LANES, width), F32)],
        compiler_params=params,
        name="ssd_forward",
    )(x_act, bc_act, step, cum, pre, grad_hidden, state_in, chan)

    stats = small_sum(stats.reshape(-1, LANES), (("tensor", 0),), 4).reshape(stats.shape)

    grad_mixed, cot_gate, hidden, ds_local, sums_n = pl.pallas_call(
        functools.partial(gating_kernel, pairs, inner_total),
        grid=grid,
        out_shape=[
            sds((batch, span, width), F32),
            sds((batch, span, width), BF),
            sds((batch, span, width), BF),
            sds((batch, LANES, width), F32),
            sds((8, width), F32),
        ],
        in_specs=[
            token_spec(width),
            token_spec(2 * LANES),
            token_spec(LANES),
            token_spec(width),
            token_spec(width),
            token_spec(width),
            pl.BlockSpec((1, 2, L), lambda n, j: (n, 0, j)),
            whole_spec((8, width)),
        ],
        out_specs=[
            token_spec(width),
            token_spec(width),
            token_spec(width),
            span_spec((LANES, width)),
            whole_spec((8, width)),
        ],
        scratch_shapes=[pltpu.VMEM((8, LANES), F32)],
        compiler_params=params,
        name="gating_backward",
    )(x_act, bc_act, cum, pre, grad_hidden, mixed, stats, chan)

    carried = chain(ds_local, tot_wide, -1, 5)

    grad_o = jnp.einsum("btd,btk->dk", cots, hidden, preferred_element_type=F32).astype(BF)
    grad_z = jnp.einsum("btd,btk->dk", normed, cot_gate, preferred_element_type=F32).astype(BF)
    grad_oz = jnp.concatenate([grad_o, grad_z], axis=1)
    carried, grad_oz = lax.optimization_barrier((carried, grad_oz))
    red_oz = lax.psum_scatter(grad_oz, pspace, scatter_dimension=0, tiled=True)
    branch_part = jnp.einsum("btk,dk->btd", hidden, full_o, preferred_element_type=F32).astype(BF)
    branch = scatter_tokens(branch_part, 1)
    block_output = jnp.swapaxes((flat_in + branch).astype(BF), 0, 1)

    cot_in, tail, sums_x, sums_bc, sums_dt = pl.pallas_call(
        functools.partial(backward_kernel, pairs),
        grid=grid,
        out_shape=[
            sds((batch, span, wide), BF),
            sds((batch, 8, tails), F32),
            sds((8, width), F32),
            sds((8, 2 * LANES), F32),
            sds((8, LANES), F32),
        ],
        in_specs=[
            token_spec(width, 0, groups),
            token_spec(width, 0, groups),
            token_spec(width, 0, groups),
            token_spec(width, 0, groups),
            token_spec(2 * LANES, 0, groups),
            token_spec(2 * LANES, 0, groups),
            token_spec(LANES, 0, groups),
            token_spec(LANES, 0, groups),
            pl.BlockSpec((1, 1, LANES, width), lambda n, j: (n, groups - 1 - j, 0, 0)),
            pl.BlockSpec((1, 1, LANES, width), lambda n, j: (n, groups - 1 - j, 0, 0)),
            token_spec(width, 0, groups),
            token_spec(width, 1, groups),
            token_spec(2 * LANES, at_bc, groups),
            token_spec(LANES, at_dt, groups),
            span_spec((8, tails)),
            span_spec((LANES, width)),
            whole_spec((8, width)),
            whole_spec((8, width)),
            whole_spec((8, 2 * LANES)),
            whole_spec((8, LANES)),
        ],
        out_specs=[
            token_spec(wide, 0, groups),
            span_spec((8, tails)),
            whole_spec((8, width)),
            whole_spec((8, 2 * LANES)),
            whole_spec((8, LANES)),
        ],
        scratch_shapes=[
            pltpu.VMEM((LANES, width), F32),
            pltpu.VMEM((L + 8, width), F32),
            pltpu.VMEM((L + 8, 2 * LANES), F32),
        ],
        compiler_params=params,
        name="ssd_backward",
    )(
        grad_mixed,
        cot_gate,
        x_act,
        ds_x,
        bc_act,
        ds_bc,
        step,
        cum,
        ent,
        aft,
        mixed,
        pre,
        pre,
        pre,
        halo,
        carried,
        chan,
        taps_x,
        taps_bc,
        small,
    )
    later = shifted(tail, -1)
    cot_in = cot_in.at[:, span - 8 :, width:].add(later.astype(BF))

    grad_wx = jnp.einsum("btd,btk->dk", normed, cot_in[..., width:], preferred_element_type=F32)
    grad_wx, cot_in = lax.optimization_barrier((grad_wx.astype(BF), cot_in))
    red_x = lax.psum_scatter(grad_wx, pspace, scatter_dimension=0, tiled=True)
    part = jnp.einsum("btk,dk->btd", cot_in, full_in, preferred_element_type=F32).astype(BF)
    grad_normed = scatter_tokens(part, 2)

    scaled = grad_normed * gain_in
    grad_base = inv_in * (scaled - base * jnp.mean(scaled * base, -1, keepdims=True))
    input_grad = jnp.swapaxes((cot_rows.astype(F32) + grad_base).astype(BF), 0, 1)
    gain_part = jnp.sum(grad_normed * base, (0, 1))

    sizes_own = (
        sums_x[:5, :inner].reshape(-1),
        sums_n[0, :inner],
        jnp.sum(sums_n[1, :inner].reshape(heads, HD), -1),
        sums_dt[0, :heads],
        sums_dt[1, :heads],
    )
    mine = rows_of_lanes(jnp.concatenate(sizes_own))
    rest = rows_of_lanes(jnp.concatenate([sums_bc[:5].reshape(-1), gain_part]))
    first = mine.shape[0]
    summed = small_sum(
        jnp.concatenate([mine, rest], 0), (("dp", 0), ("seq", 0), ("tensor", first)), 6
    )
    own, shared = summed[:first].reshape(-1), summed[first:].reshape(-1)
    part_bc = red_x[:, width : width + 2 * state_n].astype(F32)
    grad_bc = small_sum(part_bc.reshape(-1, LANES), (("tensor", 0),), 7)

    n5 = 5 * inner
    bc5 = 5 * 2 * state_n
    return (
        block_output,
        input_grad,
        shared[bc5 : bc5 + model],
        jnp.stack([red_oz[:, width : width + inner], red_x[:, :inner]], 1).astype(F32),
        grad_bc.reshape(rows_w, 2, state_n),
        red_x[:, width + 2 * state_n : width + 2 * state_n + heads].astype(F32),
        own[: 4 * inner].reshape(4, inner),
        own[4 * inner : n5],
        shared[: 4 * 2 * state_n].reshape(4, 2, state_n),
        shared[4 * 2 * state_n : bc5].reshape(2, state_n),
        own[n5 + inner + heads : n5 + inner + 2 * heads],
        own[n5 + inner + 2 * heads : n5 + inner + 3 * heads],
        own[n5 + inner : n5 + inner + heads],
        own[n5 : n5 + inner],
        red_oz[:, :inner].astype(F32),
    )


def solution(mesh):
    return jax.shard_map(
        shards,
        mesh=mesh,
        in_specs=(
            P(("seq", "tensor"), "dp", None),
            P(),
            P(("dp", "seq"), None, "tensor"),
            P(("dp", "seq"), None, None),
            P(("dp", "seq"), "tensor"),
            P(None, "tensor"),
            P("tensor"),
            P(),
            P(),
            P("tensor"),
            P("tensor"),
            P("tensor"),
            P("tensor"),
            P(("dp", "seq"), "tensor"),
            P(("seq", "tensor"), "dp", None),
        ),
        out_specs=(
            P(("seq", "tensor"), "dp", None),
            P(("seq", "tensor"), "dp", None),
            P(),
            P(("dp", "seq"), None, "tensor"),
            P(("dp", "seq"), None, None),
            P(("dp", "seq"), "tensor"),
            P(None, "tensor"),
            P("tensor"),
            P(),
            P(),
            P("tensor"),
            P("tensor"),
            P("tensor"),
            P("tensor"),
            P(("dp", "seq"), "tensor"),
        ),
        check_vma=False,
    )
```

```python
import functools

import jax
import jax.numpy as jnp
from jax import lax
from jax.experimental import pallas as pl
from jax.experimental.layout import Layout, with_layout_constraint
from jax.experimental.pallas import tpu as pltpu
from jax.sharding import PartitionSpec as P

L = 256
HD = 64
LANES = 128
EPS = 1e-05
F32 = jnp.float32
BF = jnp.bfloat16
MESH = pl.DeviceIdType.MESH
VMEM_LIMIT = 60 * 1024 * 1024
NEG = -1e30


def dot(a, b):
    return jnp.dot(a, b, preferred_element_type=F32)


def dot_nt(a, b):
    return lax.dot_general(a, b, (((1,), (1,)), ((), ())), preferred_element_type=F32)


def split(v):
    hi = v.astype(BF)
    return hi, (v - hi.astype(F32)).astype(BF)


def dot_split(mat, v):
    hi, lo = split(v)
    return dot(mat, hi) + dot(mat, lo)


def split_dot(v, mat):
    hi, lo = split(v)
    return dot(hi, mat) + dot(lo, mat)


def iota(shape, axis):
    return lax.broadcasted_iota(jnp.int32, shape, axis)


def pair_of(col, i, low):
    rows = col.shape[0]
    a = jnp.broadcast_to(col[:, 2 * i : 2 * i + 1], (rows, LANES))
    b = jnp.broadcast_to(col[:, 2 * i + 1 : 2 * i + 2], (rows, LANES))
    return jnp.where(low[:rows], a, b)


def segments(i):
    r, c = iota((LANES, LANES), 0), iota((LANES, LANES), 1)
    return jnp.where(c == 2 * i + jnp.where(r >= HD, 1, 0), 1.0, 0.0).astype(BF)


def sigmoid(v):
    return 1.0 / (1.0 + jnp.exp(-v))


def softplus(z):
    return jnp.maximum(z, 0.0) + jnp.log1p(jnp.exp(-jnp.abs(z)))


def acts_kernel(
    pairs,
    x_ref,
    bc_ref,
    dt_ref,
    halo_ref,
    cx_ref,
    cbc_ref,
    small_ref,
    xa_ref,
    dsx_ref,
    bca_ref,
    dsbc_ref,
    time_ref,
    cum_ref,
    state_ref,
    tot_ref,
    ext_x,
    ext_bc,
):
    j = pl.program_id(1)
    width = pairs * LANES

    @pl.when(j == 0)
    def _():
        ext_x[0:8, :] = halo_ref[0, :, 0:width]
        ext_bc[0:8, :] = halo_ref[0, :, width : width + 2 * LANES]
        state_ref[...] = jnp.zeros_like(state_ref)
        tot_ref[...] = jnp.zeros_like(tot_ref)

    ext_x[8 : 8 + L, :] = x_ref[0]
    ext_bc[8 : 8 + L, :] = bc_ref[0]
    low = iota((L, LANES), 1) < HD
    z = dt_ref[0] + small_ref[0:1, :]
    step = softplus(z)
    tri = jnp.where(iota((L, L), 0) >= iota((L, L), 1), 1.0, 0.0).astype(BF)
    rate = step * small_ref[1:2, :]
    r1 = rate.astype(BF)
    rest = rate - r1.astype(F32)
    r2 = rest.astype(BF)
    r3 = (rest - r2.astype(F32)).astype(BF)
    cum = dot(tri, r1) + dot(tri, r2) + dot(tri, r3)
    time_ref[0] = step
    cum_ref[0] = cum
    last = cum[L - 1 : L, :]
    tot_ref[0] = tot_ref[0] + jnp.broadcast_to(last, (8, LANES))
    decay = jnp.exp(last)
    weight = jnp.exp(last - cum) * step

    def act(ext, taps, at):
        v = taps[4:5, at] + taps[0:1, at] * ext[5 : 5 + L, at]
        for k in range(1, 4):
            v = v + taps[k : k + 1, at] * ext[5 + k : 5 + k + L, at]
        s = sigmoid(v)
        a = v * s
        return a, s * (1.0 + v * (1.0 - s))

    b_t = None
    for i in range(2):
        at = slice(i * LANES, (i + 1) * LANES)
        a, d = act(ext_bc, cbc_ref, at)
        bca_ref[0, :, at] = a
        dsbc_ref[0, :, at] = d.astype(BF)
        if i == 0:
            b_t = a.T.astype(BF)
    for i in range(pairs):
        at = slice(i * LANES, (i + 1) * LANES)
        a, d = act(ext_x, cx_ref, at)
        xa_ref[0, :, at] = a
        dsx_ref[0, :, at] = d.astype(BF)
        wx = (a * pair_of(weight, i, low)).astype(BF)
        state_ref[0, :, at] = state_ref[0, :, at] * pair_of(decay, i, low) + dot(b_t, wx)
    ext_x[0:8, :] = ext_x[L : L + 8, :]
    ext_bc[0:8, :] = ext_bc[L : L + 8, :]


def forward_kernel(
    pairs,
    x_ref,
    bc_ref,
    time_ref,
    cum_ref,
    gate_ref,
    gh_ref,
    in_ref,
    chan_ref,
    mixed_ref,
    ent_ref,
    aft_ref,
    stat_ref,
    state,
):
    j = pl.program_id(1)

    @pl.when(j == 0)
    def _():
        state[...] = in_ref[0]

    low = iota((L, LANES), 1) < HD
    b_t, b_lo = split(bc_ref[0, :, 0:LANES].T)
    c, c_lo = split(bc_ref[0, :, LANES : 2 * LANES])
    scores = dot(c, b_t) + (dot(c, b_lo) + dot(c_lo, b_t))
    step, cum = time_ref[0], cum_ref[0]
    cum_t = cum.T
    last = cum[L - 1 : L, :]
    decay = jnp.exp(last)
    grow = jnp.exp(cum)
    weight = jnp.exp(last - cum) * step
    half = L // 2
    mask = jnp.where(iota((half, half), 0) >= iota((half, half), 1), 0.0, NEG)
    squares = jnp.zeros((L, LANES), F32)
    inner = jnp.zeros((L, LANES), F32)
    for i in range(pairs):
        at = slice(i * LANES, (i + 1) * LANES)
        x = x_ref[0, :, at]
        xdt = x * pair_of(step, i, low)
        xdt_b, xdt_lo = split(xdt)
        old = state[:, at]
        old_b, old_lo = split(old)
        ent_ref[0, 0, :, at] = old_b
        y = pair_of(grow, i, low) * (dot(c, old_b) + dot(c, old_lo))
        new = old * pair_of(decay, i, low) + dot_split(b_t, x * pair_of(weight, i, low))
        state[:, at] = new
        aft_ref[0, 0, :, at] = new
        tops = jnp.zeros((half, LANES), F32)
        bots = jnp.zeros((half, LANES), F32)
        zero = jnp.zeros_like(xdt_b)
        for s in range(2):
            h = 2 * i + s
            xm = jnp.where(low, xdt_b, zero) if s == 0 else jnp.where(low, zero, xdt_b)
            xl = jnp.where(low, xdt_lo, zero) if s == 0 else jnp.where(low, zero, xdt_lo)
            top = jnp.exp(cum[:half, h : h + 1] - cum_t[h : h + 1, :half] + mask)
            mix = (top * scores[:half, :half]).astype(BF)
            tops = tops + (dot(mix, xm[:half]) + dot(mix, xl[:half]))
            left = jnp.exp(cum[half:, h : h + 1] - cum_t[h : h + 1, :half])
            right = jnp.exp(cum[half:, h : h + 1] - cum_t[h : h + 1, half:] + mask)
            mix = jnp.concatenate(
                [
                    (left * scores[half:, :half]).astype(BF),
                    (right * scores[half:, half:]).astype(BF),
                ],
                axis=1,
            )
            bots = bots + (dot(mix, xm) + dot(mix, xl))
        y = y + jnp.concatenate([tops, bots], axis=0)
        mixed = y + chan_ref[0:1, at] * x
        mixed_ref[0, :, at] = mixed
        gate = gate_ref[0, :, at]
        gated = mixed * (gate * sigmoid(gate))
        squares = squares + gated * gated
        inner = inner + gated * (gh_ref[0, :, at] * chan_ref[1:2, at])
    lane = iota((L, LANES), 1)
    both = jnp.where(
        lane == 0,
        jnp.sum(squares, axis=1, keepdims=True),
        jnp.where(lane == 1, jnp.sum(inner, axis=1, keepdims=True), 0.0),
    )
    stat_ref[0] = both.T[0:2, :]


def gating_kernel(
    pairs,
    total,
    x_ref,
    bc_ref,
    cum_ref,
    gate_ref,
    gh_ref,
    mixed_ref,
    stat_ref,
    chan_ref,
    grad_ref,
    cgate_ref,
    hidden_ref,
    ds_ref,
    sums_ref,
    before,
):
    n, j = pl.program_id(0), pl.program_id(1)

    @pl.when(j == 0)
    def _():
        before[...] = jnp.zeros_like(before)
        ds_ref[...] = jnp.zeros_like(ds_ref)

    @pl.when((j == 0) & (n == 0))
    def _():
        sums_ref[...] = jnp.zeros_like(sums_ref)

    low = iota((L, LANES), 1) < HD
    rows = iota((LANES, L), 0)
    stat = jnp.where(
        rows == 0,
        jnp.broadcast_to(stat_ref[0, 0:1, :], (LANES, L)),
        jnp.broadcast_to(stat_ref[0, 1:2, :], (LANES, L)),
    ).T
    inv = lax.rsqrt(stat[:, 0:1] * (1.0 / total) + EPS)
    back = inv * inv * inv * (stat[:, 1:2] * (1.0 / total))
    inv = jnp.broadcast_to(inv, (L, LANES))
    back = jnp.broadcast_to(back, (L, LANES))
    cum = cum_ref[0]
    grow = jnp.exp(cum + before[0:1, :])
    before[...] = before[...] + jnp.broadcast_to(cum[L - 1 : L, :], before.shape)
    c_t = bc_ref[0, :, LANES : 2 * LANES].T.astype(BF)
    for i in range(pairs):
        at = slice(i * LANES, (i + 1) * LANES)
        x = x_ref[0, :, at]
        gate = gate_ref[0, :, at]
        mixed = mixed_ref[0, :, at]
        gh = gh_ref[0, :, at]
        gain = chan_ref[1:2, at]
        sig = sigmoid(gate)
        act = gate * sig
        gated = mixed * act
        normal = gated * inv
        hidden_ref[0, :, at] = (normal * gain).astype(BF)
        grad_gated = inv * (gh * gain) - gated * back
        grad = grad_gated * act
        grad_ref[0, :, at] = grad
        cgate_ref[0, :, at] = (grad_gated * mixed * sig * (1.0 + gate * (1.0 - sig))).astype(BF)
        ds_ref[0, :, at] = ds_ref[0, :, at] + dot(
            c_t, (grad * pair_of(grow, i, low)).astype(BF)
        )
        sums_ref[0:1, at] = sums_ref[0:1, at] + jnp.sum(gh * normal, axis=0, keepdims=True)
        sums_ref[1:2, at] = sums_ref[1:2, at] + jnp.sum(grad * x, axis=0, keepdims=True)


def backward_kernel(
    pairs,
    grad_ref,
    cgate_ref,
    x_ref,
    dsx_ref,
    bc_ref,
    dsbc_ref,
    time_ref,
    cum_ref,
    ent_ref,
    aft_ref,
    mixed_ref,
    px_ref,
    pbc_ref,
    pdt_ref,
    halo_ref,
    carried_ref,
    chan_ref,
    cx_ref,
    cbc_ref,
    small_ref,
    cot_ref,
    tail_ref,
    sx_ref,
    sbc_ref,
    sdt_ref,
    state,
    ext_x,
    ext_bc,
):
    n, g = pl.program_id(0), pl.program_id(1)
    final = pl.num_programs(1) - 1
    width = pairs * LANES

    @pl.when(g == 0)
    def _():
        state[...] = carried_ref[0]
        ext_x[L : L + 8, :] = jnp.zeros((8, width), F32)
        ext_bc[L : L + 8, :] = jnp.zeros((8, 2 * LANES), F32)

    @pl.when((g == 0) & (n == 0))
    def _():
        sx_ref[...] = jnp.zeros_like(sx_ref)
        sbc_ref[...] = jnp.zeros_like(sbc_ref)
        sdt_ref[...] = jnp.zeros_like(sdt_ref)

    low = iota((L, LANES), 1) < HD
    b, b_lo = split(bc_ref[0, :, 0:LANES])
    c_full = bc_ref[0, :, LANES : 2 * LANES]
    c = c_full.astype(BF)
    c_t, c_lo = split(c_full.T)
    scores_t = dot(b, c_t) + (dot(b, c_lo) + dot(b_lo, c_t))
    step, cum = time_ref[0], cum_ref[0]
    cum_t = cum.T
    last = cum[L - 1 : L, :]
    decay = jnp.exp(last)
    grow = jnp.exp(cum)
    fade = jnp.exp(last - cum)
    half = L // 2
    mask = jnp.where(iota((half, half), 1) >= iota((half, half), 0), 0.0, NEG)
    grad_b = jnp.zeros((L, LANES), F32)
    grad_c = jnp.zeros((L, LANES), F32)
    ds_a = jnp.zeros((half, half), F32)
    ds_b = jnp.zeros((half, half), F32)
    ds_d = jnp.zeros((half, half), F32)
    dcum = jnp.zeros((L, LANES), F32)
    cols = jnp.zeros((L, LANES), F32)
    dlast = jnp.zeros((8, LANES), F32)

    for i in range(pairs):
        at = slice(i * LANES, (i + 1) * LANES)
        seg = segments(i)
        x = x_ref[0, :, at]
        dt_e = pair_of(step, i, low)
        fade_e = pair_of(fade, i, low)
        xdt = x * dt_e
        xdt_b = xdt.astype(BF)
        gm = grad_ref[0, :, at]
        gm_b, gm_lo = split(gm)
        grow_g, grow_lo = split(gm * pair_of(grow, i, low))
        ds_old = state[:, at]
        ds_old_b, ds_old_lo = split(ds_old)
        dxdt = fade_e * (dot(b, ds_old_b) + dot(b, ds_old_lo))
        grad_b = grad_b + dot_nt((xdt * fade_e).astype(BF), ds_old_b)
        grad_c = grad_c + dot_nt(grow_g, ent_ref[0, 0, :, at])
        lasts = jnp.sum(aft_ref[0, 0, :, at] * ds_old, axis=0, keepdims=True)
        dlast = dlast + split_dot(jnp.broadcast_to(lasts, (8, LANES)), seg)
        state[:, at] = ds_old * pair_of(decay, i, low) + (dot(c_t, grow_g) + dot(c_t, grow_lo))
        zero = jnp.zeros_like(xdt_b)
        tops = jnp.zeros((half, LANES), F32)
        bots = jnp.zeros((half, LANES), F32)
        for s in range(2):
            h = 2 * i + s
            xm = jnp.where(low, xdt_b, zero) if s == 0 else jnp.where(low, zero, xdt_b)
            gs = jnp.where(low, gm_b, zero) if s == 0 else jnp.where(low, zero, gm_b)
            gl = jnp.where(low, gm_lo, zero) if s == 0 else jnp.where(low, zero, gm_lo)
            row, col = cum_t[h : h + 1, :], cum[:, h : h + 1]
            low_a = jnp.exp(row[:, :half] - col[:half] + mask)
            low_b = jnp.exp(row[:, half:] - col[:half])
            low_d = jnp.exp(row[:, half:] - col[half:] + mask)
            dm_top = dot_nt(xm[:half], gm_b)
            dm_bot = dot_nt(xm[half:], gm_b[half:])
            ds_a = ds_a + dm_top[:, :half] * low_a
            ds_b = ds_b + dm_top[:, half:] * low_b
            ds_d = ds_d + dm_bot * low_d
            mix = jnp.concatenate(
                [
                    (low_a * scores_t[:half, :half]).astype(BF),
                    (low_b * scores_t[:half, half:]).astype(BF),
                ],
                axis=1,
            )
            tops = tops + (dot(mix, gs) + dot(mix, gl))
            mix = (low_d * scores_t[half:, half:]).astype(BF)
            bots = bots + (dot(mix, gs[half:]) + dot(mix, gl[half:]))
        dxdt = dxdt + jnp.concatenate([tops, bots], axis=0)
        skip = chan_ref[0:1, at]
        dcum = dcum + split_dot(gm * (mixed_ref[0, :, at] - skip * x), seg)
        cols = cols + split_dot(xdt * dxdt, seg)
        gx = (dt_e * dxdt + skip * gm) * dsx_ref[0, :, at].astype(F32)
        ext_x[0:L, at] = gx
        px = px_ref[0, :, at]
        cot = cx_ref[3:4, at] * gx
        sx_ref[3:4, at] = sx_ref[3:4, at] + jnp.sum(px * gx, axis=0, keepdims=True)
        sx_ref[4:5, at] = sx_ref[4:5, at] + jnp.sum(gx, axis=0, keepdims=True)
        for k in range(3):
            moved = ext_x[3 - k : 3 - k + L, at]
            cot = cot + cx_ref[k : k + 1, at] * moved
            sx_ref[k : k + 1, at] = sx_ref[k : k + 1, at] + jnp.sum(
                px * moved, axis=0, keepdims=True
            )
        cot_ref[0, :, at] = cgate_ref[0, :, at]
        cot_ref[0, :, width + i * LANES : width + (i + 1) * LANES] = cot.astype(BF)

    zero = jnp.zeros((half, half), F32)
    ds_t = jnp.concatenate(
        [jnp.concatenate([ds_a, ds_b], axis=1), jnp.concatenate([zero, ds_d], axis=1)], axis=0
    )
    grad_b = grad_b + dot(ds_t.astype(BF), c)
    grad_c = grad_c + dot(ds_t.T.astype(BF), b)
    for i, part in ((0, grad_b), (1, grad_c)):
        at = slice(i * LANES, (i + 1) * LANES)
        gb = part * dsbc_ref[0, :, at].astype(F32)
        ext_bc[0:L, at] = gb
        pb = pbc_ref[0, :, at]
        cot = cbc_ref[3:4, at] * gb
        sbc_ref[3:4, at] = sbc_ref[3:4, at] + jnp.sum(pb * gb, axis=0, keepdims=True)
        sbc_ref[4:5, at] = sbc_ref[4:5, at] + jnp.sum(gb, axis=0, keepdims=True)
        for k in range(3):
            moved = ext_bc[3 - k : 3 - k + L, at]
            cot = cot + cbc_ref[k : k + 1, at] * moved
            sbc_ref[k : k + 1, at] = sbc_ref[k : k + 1, at] + jnp.sum(
                pb * moved, axis=0, keepdims=True
            )
        cot_ref[0, :, 2 * width + i * LANES : 2 * width + (i + 1) * LANES] = cot.astype(BF)

    upper = jnp.where(iota((L, L), 1) >= iota((L, L), 0), 1.0, 0.0).astype(BF)
    drate = dot_split(upper, dcum - cols) + dlast[0:1, :]
    z = pdt_ref[0] + small_ref[0:1, :]
    sig = sigmoid(z)
    ratio = jnp.where(z < -15.0, 1.0, sig / jnp.where(z < -15.0, 1.0, step))
    dz = cols * ratio + drate * small_ref[1:2, :] * sig
    cot_ref[0, :, 2 * width + 2 * LANES : 2 * width + 3 * LANES] = dz.astype(BF)
    sdt_ref[0:1, :] = sdt_ref[0:1, :] + jnp.sum(dz, axis=0, keepdims=True)
    sdt_ref[1:2, :] = sdt_ref[1:2, :] + jnp.sum(
        drate * step * small_ref[1:2, :], axis=0, keepdims=True
    )

    @pl.when(g == final)
    def _():
        for ext, taps, sums, first, wide in (
            (ext_x, cx_ref, sx_ref, 0, width),
            (ext_bc, cbc_ref, sbc_ref, width, 2 * LANES),
        ):
            both = jnp.concatenate([jnp.zeros((8, wide), F32), ext[0:8, :]], axis=0)
            before = halo_ref[0, :, first : first + wide]
            total = jnp.zeros((8, wide), F32)
            for k in range(3):
                moved = both[3 - k : 11 - k, :]
                total = total + taps[k : k + 1, :] * moved
                sums[k : k + 1, :] = sums[k : k + 1, :] + jnp.sum(
                    before * moved, axis=0, keepdims=True
                )
            tail_ref[0, :, first : first + wide] = total
        tail_ref[0, :, width + 2 * LANES :] = jnp.zeros((8, LANES), F32)

    ext_x[L : L + 8, :] = ext_x[0:8, :]
    ext_bc[L : L + 8, :] = ext_bc[0:8, :]


def tensor_peers():
    me = lax.axis_index("tensor")
    chip, core = me // 2, lax.rem(me, 2)
    partner = chip * 2 + (1 - core)
    across = (1 - chip) * 2 + core
    return me, chip, core, partner, across


def greet(partner, across):
    barrier = pltpu.get_barrier_semaphore()
    for peer in (partner, across):
        pl.semaphore_signal(barrier, inc=1, device_id={"tensor": peer}, device_id_type=MESH)
    pl.semaphore_wait(barrier, 2)


def gather_kernel(cuts, count, *refs):
    ins, outs = refs[:count], refs[count : 2 * count]
    own_sem, near_s, near_r, far_s, far_r, pass_s, pass_r = refs[2 * count :]
    me, chip, core, partner, across = tensor_peers()
    greet(partner, across)
    batch, rows = ins[0].shape[0], ins[0].shape[1]
    piece = rows // cuts

    def remote(src, dst, send, recv, peer):
        return pltpu.make_async_remote_copy(
            src_ref=src,
            dst_ref=dst,
            send_sem=send,
            recv_sem=recv,
            device_id={"tensor": peer},
            device_id_type=MESH,
        )

    todo = []
    at = 0
    for a in range(count):
        for n in range(batch):
            for cut in range(cuts):
                mine = pl.ds(pl.multiple_of(me * rows + cut * piece, piece), piece)
                theirs = pl.ds(pl.multiple_of(across * rows + cut * piece, piece), piece)
                src = ins[a].at[n, cut * piece : (cut + 1) * piece, :]
                far = remote(src, outs[a].at[n, mine, :], far_s.at[at], far_r.at[at], across)
                near = remote(src, outs[a].at[n, mine, :], near_s.at[at], near_r.at[at], partner)
                own = pltpu.make_async_copy(src, outs[a].at[n, mine, :], own_sem.at[at])
                here = outs[a].at[n, theirs, :]
                onward = remote(here, here, pass_s.at[at], pass_r.at[at], partner)
                todo.append((far, near, own, onward))
                at += 1
    for far, near, own, onward in todo:
        far.start()
    for far, near, own, onward in todo:
        near.start()
        own.start()
    for far, near, own, onward in todo:
        far.wait_recv()
        onward.start()
    for far, near, own, onward in todo:
        far.wait_send()
        near.wait()
        own.wait()
        onward.wait()


def gather_tokens(*arrays):
    size = lax.axis_size("tensor")
    if size != 4:
        return [lax.all_gather(a, "tensor", axis=1, tiled=True) for a in arrays]
    batch, rows, width = arrays[0].shape
    count, cuts = len(arrays), 2
    sems = count * batch * cuts
    out = jax.ShapeDtypeStruct((batch, size * rows, width), arrays[0].dtype)
    return pl.pallas_call(
        functools.partial(gather_kernel, cuts, count),
        out_shape=[out] * count,
        in_specs=[pl.BlockSpec(memory_space=pltpu.VMEM)] * count,
        out_specs=[pl.BlockSpec(memory_space=pl.ANY)] * count,
        scratch_shapes=[pltpu.SemaphoreType.DMA((sems,))] * 7,
        compiler_params=pltpu.CompilerParams(
            collective_id=0, has_side_effects=True, vmem_limit_bytes=16 * 1024 * 1024
        ),
        name="gather_tokens",
    )(*arrays)


def scatter_kernel(cuts, in_ref, out_ref, near_buf, far_buf, sum_buf, near_s, near_r, far_s, far_r):
    me, chip, core, partner, across = tensor_peers()
    greet(partner, across)
    batch, rows = out_ref.shape[0], out_ref.shape[1]
    piece = rows // cuts

    def rows_of(owner, cut):
        return pl.ds(pl.multiple_of(owner * rows + cut * piece, piece), piece)

    def remote(src, dst, send, recv, peer):
        return pltpu.make_async_remote_copy(
            src_ref=src,
            dst_ref=dst,
            send_sem=send,
            recv_sem=recv,
            device_id={"tensor": peer},
            device_id_type=MESH,
        )

    near = {}
    for step, target in ((0, (1 - chip) * 2 + (1 - core)), (1, chip * 2 + (1 - core))):
        for n in range(batch):
            for cut in range(cuts):
                at = (step * batch + n) * cuts + cut
                near[step, n, cut] = remote(
                    in_ref.at[n, rows_of(target, cut), :],
                    near_buf.at[at],
                    near_s.at[at],
                    near_r.at[at],
                    partner,
                )
                near[step, n, cut].start()
    far = {}
    for n in range(batch):
        for cut in range(cuts):
            at = n * cuts + cut
            near[0, n, cut].wait_recv()
            sum_buf[at] = (
                in_ref[n, rows_of(across, cut), :].astype(F32) + near_buf[at].astype(F32)
            ).astype(BF)
            far[n, cut] = remote(
                sum_buf.at[at], far_buf.at[at], far_s.at[at], far_r.at[at], across
            )
            far[n, cut].start()
    for n in range(batch):
        for cut in range(cuts):
            at = n * cuts + cut
            near[1, n, cut].wait_recv()
            far[n, cut].wait_recv()
            out_ref[n, cut * piece : (cut + 1) * piece, :] = (
                in_ref[n, rows_of(me, cut), :].astype(F32)
                + near_buf[batch * cuts + at].astype(F32)
                + far_buf[at].astype(F32)
            )
    for key in near:
        near[key].wait_send()
    for key in far:
        far[key].wait_send()


def scatter_tokens(part, ident):
    size = lax.axis_size("tensor")
    if size != 4:
        return lax.psum_scatter(part, "tensor", scatter_dimension=1, tiled=True).astype(F32)
    batch, tokens, width = part.shape
    rows, cuts = tokens // size, 2
    piece = rows // cuts
    return pl.pallas_call(
        functools.partial(scatter_kernel, cuts),
        out_shape=jax.ShapeDtypeStruct((batch, rows, width), F32),
        in_specs=[pl.BlockSpec(memory_space=pltpu.VMEM)],
        out_specs=pl.BlockSpec(memory_space=pltpu.VMEM),
        scratch_shapes=[
            pltpu.VMEM((2 * batch * cuts, piece, width), BF),
            pltpu.VMEM((batch * cuts, piece, width), BF),
            pltpu.VMEM((batch * cuts, piece, width), BF),
            pltpu.SemaphoreType.DMA((2 * batch * cuts,)),
            pltpu.SemaphoreType.DMA((2 * batch * cuts,)),
            pltpu.SemaphoreType.DMA((batch * cuts,)),
            pltpu.SemaphoreType.DMA((batch * cuts,)),
        ],
        compiler_params=pltpu.CompilerParams(
            collective_id=ident, has_side_effects=True, vmem_limit_bytes=40 * 1024 * 1024
        ),
        name="scatter_tokens",
    )(part)


def chain_kernel(by, cuts, own_ref, tot_ref, out_ref, in_buf, send_buf, send_sem, recv_sem):
    me, size = lax.axis_index("seq"), lax.axis_size("seq")
    ahead, behind = me + by, me - by
    has_next = (ahead >= 0) & (ahead < size)
    has_prev = (behind >= 0) & (behind < size)
    barrier = pltpu.get_barrier_semaphore()

    @pl.when(has_next)
    def _():
        pl.semaphore_signal(barrier, inc=1, device_id={"seq": ahead}, device_id_type=MESH)

    @pl.when(has_prev)
    def _():
        pl.semaphore_signal(barrier, inc=1, device_id={"seq": behind}, device_id_type=MESH)

    pl.semaphore_wait(barrier, has_next.astype(jnp.int32) + has_prev.astype(jnp.int32))

    batch, rows = own_ref.shape[0], own_ref.shape[1] // cuts
    copies = []
    for n in range(batch):
        decay = jnp.exp(tot_ref[n, 0:1, :])
        for cut in range(cuts):
            at = n * cuts + cut
            here = slice(cut * rows, (cut + 1) * rows)
            copy = pltpu.make_async_remote_copy(
                src_ref=send_buf.at[at],
                dst_ref=in_buf.at[at],
                send_sem=send_sem.at[at],
                recv_sem=recv_sem.at[at],
                device_id={"seq": ahead},
                device_id_type=MESH,
            )
            copies.append(copy)

            @pl.when(has_prev)
            def _():
                copy.wait_recv()
                out_ref[n, here, :] = in_buf[at].astype(F32)

            @pl.when(jnp.logical_not(has_prev))
            def _():
                out_ref[n, here, :] = jnp.zeros((rows, out_ref.shape[2]), F32)

            @pl.when(has_next)
            def _():
                send_buf[at] = (out_ref[n, here, :] * decay + own_ref[n, here, :]).astype(BF)
                copy.start()

    @pl.when(has_next)
    def _():
        for copy in copies:
            copy.wait_send()


def chain(own, tot, by, ident):
    batch, rows, width = own.shape
    cuts = 4
    return pl.pallas_call(
        functools.partial(chain_kernel, by, cuts),
        out_shape=jax.ShapeDtypeStruct(own.shape, F32),
        in_specs=[pl.BlockSpec(memory_space=pltpu.VMEM)] * 2,
        out_specs=pl.BlockSpec(memory_space=pltpu.VMEM),
        scratch_shapes=[
            pltpu.VMEM((batch * cuts, rows // cuts, width), BF),
            pltpu.VMEM((batch * cuts, rows // cuts, width), BF),
            pltpu.SemaphoreType.DMA((batch * cuts,)),
            pltpu.SemaphoreType.DMA((batch * cuts,)),
        ],
        compiler_params=pltpu.CompilerParams(collective_id=ident, has_side_effects=True),
        name="chain",
    )(own, tot)


def sum_kernel(phases, in_ref, out_ref, *scratch):
    count = len(phases)
    bufs, sends, recvs = scratch[:count], scratch[count : 2 * count], scratch[2 * count :]
    barrier = pltpu.get_barrier_semaphore()
    greeted = 0
    for axis, _ in phases:
        me, size = lax.axis_index(axis), lax.axis_size(axis)
        for d in range(1, size):
            peer = lax.rem(me + d, size)
            pl.semaphore_signal(barrier, inc=1, device_id={axis: peer}, device_id_type=MESH)
            greeted += 1
    pl.semaphore_wait(barrier, greeted)
    out_ref[...] = in_ref[...]
    for p, (axis, first) in enumerate(phases):
        me, size = lax.axis_index(axis), lax.axis_size(axis)
        rows = in_ref.shape[0] - first
        bufs[p][pl.ds(me, 1)] = out_ref[first:, :].reshape(1, rows, LANES)
        copies = []
        for d in range(1, size):
            copies.append(
                pltpu.make_async_remote_copy(
                    src_ref=(in_ref if p == 0 else out_ref).at[pl.ds(first, rows), :],
                    dst_ref=bufs[p].at[me],
                    send_sem=sends[p].at[d - 1],
                    recv_sem=recvs[p].at[d - 1],
                    device_id={axis: lax.rem(me + d, size)},
                    device_id_type=MESH,
                )
            )
            copies[-1].start()
        for copy in copies:
            copy.wait()
        total = bufs[p][0]
        for r in range(1, size):
            total = total + bufs[p][r]
        out_ref[first:, :] = total


def small_sum(value, phases, ident):
    rows = value.shape[0]
    sizes = [lax.axis_size(axis) for axis, _ in phases]
    scratch = [pltpu.VMEM((n, rows - first, LANES), F32) for n, (_, first) in zip(sizes, phases)]
    scratch += [pltpu.SemaphoreType.DMA((max(n - 1, 1),)) for n in sizes] * 2
    return pl.pallas_call(
        functools.partial(sum_kernel, phases),
        out_shape=jax.ShapeDtypeStruct(value.shape, F32),
        in_specs=[pl.BlockSpec(memory_space=pltpu.VMEM)],
        out_specs=pl.BlockSpec(memory_space=pltpu.VMEM),
        scratch_shapes=scratch,
        compiler_params=pltpu.CompilerParams(collective_id=ident, has_side_effects=True),
        name="small_sum",
    )(value)


def rows_of_lanes(flat, unit=8 * LANES):
    short = -flat.shape[0] % unit
    return jnp.pad(flat, (0, short)).reshape(-1, LANES)


def shifted(value, by):
    peers = lax.axis_size("seq")
    pairs = [(i, i + by) for i in range(peers) if 0 <= i + by < peers]
    return lax.ppermute(value, "seq", pairs)


def pad_last(value, to):
    short = to - value.shape[-1]
    if short == 0:
        return value
    return jnp.pad(value, [(0, 0)] * (value.ndim - 1) + [(0, short)])


def token_spec(width, col=0, flip=None):
    if flip is None:
        return pl.BlockSpec((1, L, width), lambda n, j: (n, j, col))
    return pl.BlockSpec((1, L, width), lambda n, j: (n, flip - 1 - j, col))


def span_spec(shape):
    return pl.BlockSpec((1,) + shape, lambda n, j: (n,) + (0,) * len(shape))


def whole_spec(shape):
    return pl.BlockSpec(shape, lambda n, j: (0,) * len(shape))


def shards(
    block_input,
    gain_in,
    w_zx,
    w_bc,
    w_dt,
    conv_x,
    conv_x_b,
    conv_bc,
    conv_bc_b,
    dt_bias,
    a_log,
    d_skip,
    gain_norm,
    w_out,
    cotangent,
):
    rows_dev, batch, model = block_input.shape
    tensor_count = lax.axis_size("tensor")
    span = rows_dev * tensor_count
    groups = span // L
    heads = dt_bias.shape[0]
    inner = gain_norm.shape[0]
    inner_total = inner * tensor_count
    state_n = conv_bc.shape[2]
    pairs = (heads + 1) // 2
    width = pairs * LANES
    tails = width + 3 * LANES
    wide = width + tails
    rows_w = w_out.shape[0]
    pspace = ("dp", "seq")

    mine_in = jnp.concatenate(
        [
            pad_last(w_zx[:, 0], width),
            pad_last(w_zx[:, 1], width),
            w_bc.reshape(rows_w, 2 * state_n),
            pad_last(w_dt, LANES),
        ],
        axis=1,
    )
    mine_o = pad_last(w_out, width)
    full_in = lax.all_gather(mine_in, pspace, axis=0, tiled=True)
    full_in, mine_o = lax.optimization_barrier((full_in, mine_o))
    full_o = lax.all_gather(mine_o, pspace, axis=0, tiled=True)

    flat_in = jnp.swapaxes(block_input, 0, 1).astype(F32)
    cot_rows = jnp.swapaxes(cotangent, 0, 1)
    inv_in = lax.rsqrt(jnp.mean(flat_in * flat_in, -1, keepdims=True) + EPS)
    base = flat_in * inv_in
    normed_rows = (base * gain_in).astype(BF)
    normed, cots = gather_tokens(normed_rows, cot_rows)
    halo_rows = shifted(normed[:, span - 8 :], 1)

    taps_x = pad_last(jnp.concatenate([conv_x, conv_x_b[None], jnp.zeros((3, inner), F32)], 0), width)
    taps_bc = jnp.concatenate(
        [
            conv_bc.reshape(4, 2 * state_n),
            conv_bc_b.reshape(1, 2 * state_n),
            jnp.zeros((3, 2 * state_n), F32),
        ],
        0,
    )
    small = pad_last(jnp.stack([dt_bias, -jnp.exp(a_log)] + [jnp.zeros_like(a_log)] * 6), LANES)
    chan = pad_last(
        jnp.stack([jnp.repeat(d_skip, HD), gain_norm] + [jnp.zeros_like(gain_norm)] * 6), width
    )

    pre = jnp.einsum("btd,dk->btk", normed, full_in, preferred_element_type=F32)
    halo = jnp.einsum("btd,dk->btk", halo_rows, full_in[:, width:], preferred_element_type=F32)
    grad_hidden = jnp.einsum("btd,dk->btk", cots, full_o, preferred_element_type=F32)

    params = pltpu.CompilerParams(
        dimension_semantics=("arbitrary", "arbitrary"), vmem_limit_bytes=VMEM_LIMIT
    )
    grid = (batch, groups)
    at_bc, at_dt = pairs, 2 * pairs + 2
    sds = jax.ShapeDtypeStruct
    x_act, ds_x, bc_act, ds_bc, step, cum, local_state, tot = pl.pallas_call(
        functools.partial(acts_kernel, pairs),
        grid=grid,
        out_shape=[
            sds((batch, span, width), F32),
            sds((batch, span, width), BF),
            sds((batch, span, 2 * LANES), F32),
            sds((batch, span, 2 * LANES), BF),
            sds((batch, span, LANES), F32),
            sds((batch, span, LANES), F32),
            sds((batch, LANES, width), F32),
            sds((batch, 8, LANES), F32),
        ],
        in_specs=[
            token_spec(width, 1),
            token_spec(2 * LANES, at_bc),
            token_spec(LANES, at_dt),
            span_spec((8, tails)),
            whole_spec((8, width)),
            whole_spec((8, 2 * LANES)),
            whole_spec((8, LANES)),
        ],
        out_specs=[
            token_spec(width),
            token_spec(width),
            token_spec(2 * LANES),
            token_spec(2 * LANES),
            token_spec(LANES),
            token_spec(LANES),
            span_spec((LANES, width)),
            span_spec((8, LANES)),
        ],
        scratch_shapes=[pltpu.VMEM((L + 8, width), F32), pltpu.VMEM((L + 8, 2 * LANES), F32)],
        compiler_params=params,
        name="acts",
    )(pre, pre, pre, halo, taps_x, taps_bc, small)

    tot_wide = jnp.repeat(tot[:, :, : 2 * pairs], HD, axis=-1)
    state_in = chain(local_state, tot_wide, 1, 3)

    mixed, ent, aft, stats = pl.pallas_call(
        functools.partial(forward_kernel, pairs),
        grid=grid,
        out_shape=[
            sds((batch, span, width), F32),
            sds((batch, groups, LANES, width), BF),
            sds((batch, groups, LANES, width), F32),
            sds((batch, 2, span), F32),
        ],
        in_specs=[
            token_spec(width),
            token_spec(2 * LANES),
            token_spec(LANES),
            token_spec(LANES),
            token_spec(width),
            token_spec(width),
            span_spec((LANES, width)),
            whole_spec((8, width)),
        ],
        out_specs=[
            token_spec(width),
            pl.BlockSpec((1, 1, LANES, width), lambda n, j: (n, j, 0, 0)),
            pl.BlockSpec((1, 1, LANES, width), lambda n, j: (n, j, 0, 0)),
            pl.BlockSpec((1, 2, L), lambda n, j: (n, 0, j)),
        ],
        scratch_shapes=[pltpu.VMEM((LANES, width), F32)],
        compiler_params=params,
        name="ssd_forward",
    )(x_act, bc_act, step, cum, pre, grad_hidden, state_in, chan)

    stats = small_sum(stats.reshape(-1, LANES), (("tensor", 0),), 4).reshape(stats.shape)

    grad_mixed, cot_gate, hidden, ds_local, sums_n = pl.pallas_call(
        functools.partial(gating_kernel, pairs, inner_total),
        grid=grid,
        out_shape=[
            sds((batch, span, width), F32),
            sds((batch, span, width), BF),
            sds((batch, span, width), BF),
            sds((batch, LANES, width), F32),
            sds((8, width), F32),
        ],
        in_specs=[
            token_spec(width),
            token_spec(2 * LANES),
            token_spec(LANES),
            token_spec(width),
            token_spec(width),
            token_spec(width),
            pl.BlockSpec((1, 2, L), lambda n, j: (n, 0, j)),
            whole_spec((8, width)),
        ],
        out_specs=[
            token_spec(width),
            token_spec(width),
            token_spec(width),
            span_spec((LANES, width)),
            whole_spec((8, width)),
        ],
        scratch_shapes=[pltpu.VMEM((8, LANES), F32)],
        compiler_params=params,
        name="gating_backward",
    )(x_act, bc_act, cum, pre, grad_hidden, mixed, stats, chan)

    carried = chain(ds_local, tot_wide, -1, 5)

    grad_o = jnp.einsum("btd,btk->dk", cots, hidden, preferred_element_type=F32).astype(BF)
    grad_z = jnp.einsum("btd,btk->dk", normed, cot_gate, preferred_element_type=F32).astype(BF)
    grad_oz = with_layout_constraint(
        jnp.concatenate([grad_o, grad_z], axis=1), Layout(major_to_minor=(0, 1))
    )
    carried, grad_oz = lax.optimization_barrier((carried, grad_oz))
    red_oz = lax.psum_scatter(grad_oz, pspace, scatter_dimension=0, tiled=True)
    branch_part = jnp.einsum("btk,dk->btd", hidden, full_o, preferred_element_type=F32).astype(BF)
    branch = scatter_tokens(branch_part, 1)

    cot_in, tail, sums_x, sums_bc, sums_dt = pl.pallas_call(
        functools.partial(backward_kernel, pairs),
        grid=grid,
        out_shape=[
            sds((batch, span, wide), BF),
            sds((batch, 8, tails), F32),
            sds((8, width), F32),
            sds((8, 2 * LANES), F32),
            sds((8, LANES), F32),
        ],
        in_specs=[
            token_spec(width, 0, groups),
            token_spec(width, 0, groups),
            token_spec(width, 0, groups),
            token_spec(width, 0, groups),
            token_spec(2 * LANES, 0, groups),
            token_spec(2 * LANES, 0, groups),
            token_spec(LANES, 0, groups),
            token_spec(LANES, 0, groups),
            pl.BlockSpec((1, 1, LANES, width), lambda n, j: (n, groups - 1 - j, 0, 0)),
            pl.BlockSpec((1, 1, LANES, width), lambda n, j: (n, groups - 1 - j, 0, 0)),
            token_spec(width, 0, groups),
            token_spec(width, 1, groups),
            token_spec(2 * LANES, at_bc, groups),
            token_spec(LANES, at_dt, groups),
            span_spec((8, tails)),
            span_spec((LANES, width)),
            whole_spec((8, width)),
            whole_spec((8, width)),
            whole_spec((8, 2 * LANES)),
            whole_spec((8, LANES)),
        ],
        out_specs=[
            token_spec(wide, 0, groups),
            span_spec((8, tails)),
            whole_spec((8, width)),
            whole_spec((8, 2 * LANES)),
            whole_spec((8, LANES)),
        ],
        scratch_shapes=[
            pltpu.VMEM((LANES, width), F32),
            pltpu.VMEM((L + 8, width), F32),
            pltpu.VMEM((L + 8, 2 * LANES), F32),
        ],
        compiler_params=params,
        name="ssd_backward",
    )(
        grad_mixed,
        cot_gate,
        x_act,
        ds_x,
        bc_act,
        ds_bc,
        step,
        cum,
        ent,
        aft,
        mixed,
        pre,
        pre,
        pre,
        halo,
        carried,
        chan,
        taps_x,
        taps_bc,
        small,
    )
    later = shifted(tail, -1)
    cot_in = cot_in.at[:, span - 8 :, width:].add(later.astype(BF))

    grad_wx = jnp.einsum("btd,btk->dk", normed, cot_in[..., width:], preferred_element_type=F32)
    grad_wx, cot_in, red_oz, branch = lax.optimization_barrier(
        (grad_wx.astype(BF), cot_in, red_oz, branch)
    )
    block_output = jnp.swapaxes((flat_in + branch).astype(BF), 0, 1)
    red_x = lax.psum_scatter(grad_wx, pspace, scatter_dimension=0, tiled=True)
    part = jnp.einsum("btk,dk->btd", cot_in, full_in, preferred_element_type=F32).astype(BF)
    grad_normed = scatter_tokens(part, 2)

    scaled = grad_normed * gain_in
    grad_base = inv_in * (scaled - base * jnp.mean(scaled * base, -1, keepdims=True))
    input_grad = jnp.swapaxes((cot_rows.astype(F32) + grad_base).astype(BF), 0, 1)
    gain_part = jnp.sum(grad_normed * base, (0, 1))

    sizes_own = (
        sums_x[:5, :inner].reshape(-1),
        sums_n[0, :inner],
        jnp.sum(sums_n[1, :inner].reshape(heads, HD), -1),
        sums_dt[0, :heads],
        sums_dt[1, :heads],
    )
    mine = rows_of_lanes(jnp.concatenate(sizes_own))
    rest = rows_of_lanes(jnp.concatenate([sums_bc[:5].reshape(-1), gain_part]))
    first = mine.shape[0]
    summed = small_sum(
        jnp.concatenate([mine, rest], 0), (("dp", 0), ("seq", 0), ("tensor", first)), 6
    )
    own, shared = summed[:first].reshape(-1), summed[first:].reshape(-1)
    part_bc = red_x[:, width : width + 2 * state_n].astype(F32)
    grad_bc = small_sum(part_bc.reshape(-1, LANES), (("tensor", 0),), 7)

    n5 = 5 * inner
    bc5 = 5 * 2 * state_n
    return (
        block_output,
        input_grad,
        shared[bc5 : bc5 + model],
        jnp.stack([red_oz[:, width : width + inner], red_x[:, :inner]], 1).astype(F32),
        grad_bc.reshape(rows_w, 2, state_n),
        red_x[:, width + 2 * state_n : width + 2 * state_n + heads].astype(F32),
        own[: 4 * inner].reshape(4, inner),
        own[4 * inner : n5],
        shared[: 4 * 2 * state_n].reshape(4, 2, state_n),
        shared[4 * 2 * state_n : bc5].reshape(2, state_n),
        own[n5 + inner + heads : n5 + inner + 2 * heads],
        own[n5 + inner + 2 * heads : n5 + inner + 3 * heads],
        own[n5 + inner : n5 + inner + heads],
        own[n5 : n5 + inner],
        red_oz[:, :inner].astype(F32),
    )


def solution(mesh):
    return jax.shard_map(
        shards,
        mesh=mesh,
        in_specs=(
            P(("seq", "tensor"), "dp", None),
            P(),
            P(("dp", "seq"), None, "tensor"),
            P(("dp", "seq"), None, None),
            P(("dp", "seq"), "tensor"),
            P(None, "tensor"),
            P("tensor"),
            P(),
            P(),
            P("tensor"),
            P("tensor"),
            P("tensor"),
            P("tensor"),
            P(("dp", "seq"), "tensor"),
            P(("seq", "tensor"), "dp", None),
        ),
        out_specs=(
            P(("seq", "tensor"), "dp", None),
            P(("seq", "tensor"), "dp", None),
            P(),
            P(("dp", "seq"), None, "tensor"),
            P(("dp", "seq"), None, None),
            P(("dp", "seq"), "tensor"),
            P(None, "tensor"),
            P("tensor"),
            P(),
            P(),
            P("tensor"),
            P("tensor"),
            P("tensor"),
            P("tensor"),
            P(("dp", "seq"), "tensor"),
        ),
        check_vma=False,
    )
```

```python
import functools

import jax
import jax.numpy as jnp
from jax import lax
from jax.experimental import pallas as pl
from jax.experimental.layout import Layout, with_layout_constraint
from jax.experimental.pallas import tpu as pltpu
from jax.sharding import PartitionSpec as P

L = 256
HD = 64
LANES = 128
EPS = 1e-05
F32 = jnp.float32
BF = jnp.bfloat16
MESH = pl.DeviceIdType.MESH
VMEM_LIMIT = 60 * 1024 * 1024
NEG = -1e30


def dot(a, b):
    return jnp.dot(a, b, preferred_element_type=F32)


def dot_nt(a, b):
    return lax.dot_general(a, b, (((1,), (1,)), ((), ())), preferred_element_type=F32)


def split(v):
    hi = v.astype(BF)
    return hi, (v - hi.astype(F32)).astype(BF)


def dot_split(mat, v):
    hi, lo = split(v)
    return dot(mat, hi) + dot(mat, lo)


def split_dot(v, mat):
    hi, lo = split(v)
    return dot(hi, mat) + dot(lo, mat)


def iota(shape, axis):
    return lax.broadcasted_iota(jnp.int32, shape, axis)


def pair_of(col, i, low):
    rows = col.shape[0]
    a = jnp.broadcast_to(col[:, 2 * i : 2 * i + 1], (rows, LANES))
    b = jnp.broadcast_to(col[:, 2 * i + 1 : 2 * i + 2], (rows, LANES))
    return jnp.where(low[:rows], a, b)


def segments(i):
    r, c = iota((LANES, LANES), 0), iota((LANES, LANES), 1)
    return jnp.where(c == 2 * i + jnp.where(r >= HD, 1, 0), 1.0, 0.0).astype(BF)


def sigmoid(v):
    return 1.0 / (1.0 + jnp.exp(-v))


def softplus(z):
    return jnp.maximum(z, 0.0) + jnp.log1p(jnp.exp(-jnp.abs(z)))


def acts_kernel(
    pairs,
    x_ref,
    bc_ref,
    dt_ref,
    halo_ref,
    cx_ref,
    cbc_ref,
    small_ref,
    xa_ref,
    dsx_ref,
    bca_ref,
    dsbc_ref,
    time_ref,
    cum_ref,
    state_ref,
    tot_ref,
    ext_x,
    ext_bc,
):
    j = pl.program_id(1)
    width = pairs * LANES

    @pl.when(j == 0)
    def _():
        ext_x[0:8, :] = halo_ref[0, :, 0:width]
        ext_bc[0:8, :] = halo_ref[0, :, width : width + 2 * LANES]
        state_ref[...] = jnp.zeros_like(state_ref)
        tot_ref[...] = jnp.zeros_like(tot_ref)

    ext_x[8 : 8 + L, :] = x_ref[0]
    ext_bc[8 : 8 + L, :] = bc_ref[0]
    low = iota((L, LANES), 1) < HD
    z = dt_ref[0] + small_ref[0:1, :]
    step = softplus(z)
    tri = jnp.where(iota((L, L), 0) >= iota((L, L), 1), 1.0, 0.0).astype(BF)
    rate = step * small_ref[1:2, :]
    r1 = rate.astype(BF)
    rest = rate - r1.astype(F32)
    r2 = rest.astype(BF)
    r3 = (rest - r2.astype(F32)).astype(BF)
    cum = dot(tri, r1) + dot(tri, r2) + dot(tri, r3)
    time_ref[0] = step
    cum_ref[0] = cum
    last = cum[L - 1 : L, :]
    tot_ref[0] = tot_ref[0] + jnp.broadcast_to(last, (8, LANES))
    decay = jnp.exp(last)
    weight = jnp.exp(last - cum) * step

    def act(ext, taps, at):
        v = taps[4:5, at] + taps[0:1, at] * ext[5 : 5 + L, at]
        for k in range(1, 4):
            v = v + taps[k : k + 1, at] * ext[5 + k : 5 + k + L, at]
        s = sigmoid(v)
        a = v * s
        return a, s * (1.0 + v * (1.0 - s))

    b_t = None
    for i in range(2):
        at = slice(i * LANES, (i + 1) * LANES)
        a, d = act(ext_bc, cbc_ref, at)
        bca_ref[0, :, at] = a
        dsbc_ref[0, :, at] = d.astype(BF)
        if i == 0:
            b_t = a.T.astype(BF)
    for i in range(pairs):
        at = slice(i * LANES, (i + 1) * LANES)
        a, d = act(ext_x, cx_ref, at)
        xa_ref[0, :, at] = a
        dsx_ref[0, :, at] = d.astype(BF)
        wx = (a * pair_of(weight, i, low)).astype(BF)
        state_ref[0, :, at] = state_ref[0, :, at] * pair_of(decay, i, low) + dot(b_t, wx)
    ext_x[0:8, :] = ext_x[L : L + 8, :]
    ext_bc[0:8, :] = ext_bc[L : L + 8, :]


def forward_kernel(
    pairs,
    x_ref,
    bc_ref,
    time_ref,
    cum_ref,
    gate_ref,
    gh_ref,
    in_ref,
    chan_ref,
    mixed_ref,
    ent_ref,
    aft_ref,
    stat_ref,
    state,
):
    j = pl.program_id(1)

    @pl.when(j == 0)
    def _():
        state[...] = in_ref[0]

    low = iota((L, LANES), 1) < HD
    b_t, b_lo = split(bc_ref[0, :, 0:LANES].T)
    c, c_lo = split(bc_ref[0, :, LANES : 2 * LANES])
    scores = dot(c, b_t) + (dot(c, b_lo) + dot(c_lo, b_t))
    step, cum = time_ref[0], cum_ref[0]
    cum_t = cum.T
    last = cum[L - 1 : L, :]
    decay = jnp.exp(last)
    grow = jnp.exp(cum)
    weight = jnp.exp(last - cum) * step
    half = L // 2
    mask = jnp.where(iota((half, half), 0) >= iota((half, half), 1), 0.0, NEG)
    squares = jnp.zeros((L, LANES), F32)
    inner = jnp.zeros((L, LANES), F32)
    for i in range(pairs):
        at = slice(i * LANES, (i + 1) * LANES)
        x = x_ref[0, :, at]
        xdt = x * pair_of(step, i, low)
        xdt_b, xdt_lo = split(xdt)
        old = state[:, at]
        old_b, old_lo = split(old)
        ent_ref[0, 0, :, at] = old_b
        y = pair_of(grow, i, low) * (dot(c, old_b) + dot(c, old_lo))
        new = old * pair_of(decay, i, low) + dot_split(b_t, x * pair_of(weight, i, low))
        state[:, at] = new
        aft_ref[0, 0, :, at] = new
        tops = jnp.zeros((half, LANES), F32)
        bots = jnp.zeros((half, LANES), F32)
        zero = jnp.zeros_like(xdt_b)
        for s in range(2):
            h = 2 * i + s
            xm = jnp.where(low, xdt_b, zero) if s == 0 else jnp.where(low, zero, xdt_b)
            xl = jnp.where(low, xdt_lo, zero) if s == 0 else jnp.where(low, zero, xdt_lo)
            top = jnp.exp(cum[:half, h : h + 1] - cum_t[h : h + 1, :half] + mask)
            mix = (top * scores[:half, :half]).astype(BF)
            tops = tops + (dot(mix, xm[:half]) + dot(mix, xl[:half]))
            left = jnp.exp(cum[half:, h : h + 1] - cum_t[h : h + 1, :half])
            right = jnp.exp(cum[half:, h : h + 1] - cum_t[h : h + 1, half:] + mask)
            mix = jnp.concatenate(
                [
                    (left * scores[half:, :half]).astype(BF),
                    (right * scores[half:, half:]).astype(BF),
                ],
                axis=1,
            )
            bots = bots + (dot(mix, xm) + dot(mix, xl))
        y = y + jnp.concatenate([tops, bots], axis=0)
        mixed = y + chan_ref[0:1, at] * x
        mixed_ref[0, :, at] = mixed
        gate = gate_ref[0, :, at]
        gated = mixed * (gate * sigmoid(gate))
        squares = squares + gated * gated
        inner = inner + gated * (gh_ref[0, :, at] * chan_ref[1:2, at])
    lane = iota((L, LANES), 1)
    both = jnp.where(
        lane == 0,
        jnp.sum(squares, axis=1, keepdims=True),
        jnp.where(lane == 1, jnp.sum(inner, axis=1, keepdims=True), 0.0),
    )
    stat_ref[0] = both.T[0:2, :]


def gating_kernel(
    pairs,
    total,
    x_ref,
    bc_ref,
    cum_ref,
    gate_ref,
    gh_ref,
    mixed_ref,
    stat_ref,
    chan_ref,
    grad_ref,
    cgate_ref,
    hidden_ref,
    ds_ref,
    sums_ref,
    before,
):
    n, j = pl.program_id(0), pl.program_id(1)

    @pl.when(j == 0)
    def _():
        before[...] = jnp.zeros_like(before)
        ds_ref[...] = jnp.zeros_like(ds_ref)

    @pl.when((j == 0) & (n == 0))
    def _():
        sums_ref[...] = jnp.zeros_like(sums_ref)

    low = iota((L, LANES), 1) < HD
    rows = iota((LANES, L), 0)
    stat = jnp.where(
        rows == 0,
        jnp.broadcast_to(stat_ref[0, 0:1, :], (LANES, L)),
        jnp.broadcast_to(stat_ref[0, 1:2, :], (LANES, L)),
    ).T
    inv = lax.rsqrt(stat[:, 0:1] * (1.0 / total) + EPS)
    back = inv * inv * inv * (stat[:, 1:2] * (1.0 / total))
    inv = jnp.broadcast_to(inv, (L, LANES))
    back = jnp.broadcast_to(back, (L, LANES))
    cum = cum_ref[0]
    grow = jnp.exp(cum + before[0:1, :])
    before[...] = before[...] + jnp.broadcast_to(cum[L - 1 : L, :], before.shape)
    c_t = bc_ref[0, :, LANES : 2 * LANES].T.astype(BF)
    for i in range(pairs):
        at = slice(i * LANES, (i + 1) * LANES)
        x = x_ref[0, :, at]
        gate = gate_ref[0, :, at]
        mixed = mixed_ref[0, :, at]
        gh = gh_ref[0, :, at]
        gain = chan_ref[1:2, at]
        sig = sigmoid(gate)
        act = gate * sig
        gated = mixed * act
        normal = gated * inv
        hidden_ref[0, :, at] = (normal * gain).astype(BF)
        grad_gated = inv * (gh * gain) - gated * back
        grad = grad_gated * act
        grad_ref[0, :, at] = grad
        cgate_ref[0, :, at] = (grad_gated * mixed * sig * (1.0 + gate * (1.0 - sig))).astype(BF)
        ds_ref[0, :, at] = ds_ref[0, :, at] + dot(
            c_t, (grad * pair_of(grow, i, low)).astype(BF)
        )
        sums_ref[0:1, at] = sums_ref[0:1, at] + jnp.sum(gh * normal, axis=0, keepdims=True)
        sums_ref[1:2, at] = sums_ref[1:2, at] + jnp.sum(grad * x, axis=0, keepdims=True)


def backward_kernel(
    pairs,
    grad_ref,
    cgate_ref,
    x_ref,
    dsx_ref,
    bc_ref,
    dsbc_ref,
    time_ref,
    cum_ref,
    ent_ref,
    aft_ref,
    mixed_ref,
    px_ref,
    pbc_ref,
    pdt_ref,
    halo_ref,
    carried_ref,
    chan_ref,
    cx_ref,
    cbc_ref,
    small_ref,
    cot_ref,
    tail_ref,
    sx_ref,
    sbc_ref,
    sdt_ref,
    state,
    ext_x,
    ext_bc,
):
    n, g = pl.program_id(0), pl.program_id(1)
    final = pl.num_programs(1) - 1
    width = pairs * LANES

    @pl.when(g == 0)
    def _():
        state[...] = carried_ref[0]
        ext_x[L : L + 8, :] = jnp.zeros((8, width), F32)
        ext_bc[L : L + 8, :] = jnp.zeros((8, 2 * LANES), F32)

    @pl.when((g == 0) & (n == 0))
    def _():
        sx_ref[...] = jnp.zeros_like(sx_ref)
        sbc_ref[...] = jnp.zeros_like(sbc_ref)
        sdt_ref[...] = jnp.zeros_like(sdt_ref)

    low = iota((L, LANES), 1) < HD
    b, b_lo = split(bc_ref[0, :, 0:LANES])
    c_full = bc_ref[0, :, LANES : 2 * LANES]
    c = c_full.astype(BF)
    c_t, c_lo = split(c_full.T)
    scores_t = dot(b, c_t) + (dot(b, c_lo) + dot(b_lo, c_t))
    step, cum = time_ref[0], cum_ref[0]
    cum_t = cum.T
    last = cum[L - 1 : L, :]
    decay = jnp.exp(last)
    grow = jnp.exp(cum)
    fade = jnp.exp(last - cum)
    half = L // 2
    mask = jnp.where(iota((half, half), 1) >= iota((half, half), 0), 0.0, NEG)
    grad_b = jnp.zeros((L, LANES), F32)
    grad_c = jnp.zeros((L, LANES), F32)
    ds_a = jnp.zeros((half, half), F32)
    ds_b = jnp.zeros((half, half), F32)
    ds_d = jnp.zeros((half, half), F32)
    dcum = jnp.zeros((L, LANES), F32)
    cols = jnp.zeros((L, LANES), F32)
    dlast = jnp.zeros((8, LANES), F32)

    for i in range(pairs):
        at = slice(i * LANES, (i + 1) * LANES)
        seg = segments(i)
        x = x_ref[0, :, at]
        dt_e = pair_of(step, i, low)
        fade_e = pair_of(fade, i, low)
        xdt = x * dt_e
        xdt_b = xdt.astype(BF)
        gm = grad_ref[0, :, at]
        gm_b, gm_lo = split(gm)
        grow_g, grow_lo = split(gm * pair_of(grow, i, low))
        ds_old = state[:, at]
        ds_old_b, ds_old_lo = split(ds_old)
        dxdt = fade_e * (dot(b, ds_old_b) + dot(b, ds_old_lo))
        grad_b = grad_b + dot_nt((xdt * fade_e).astype(BF), ds_old_b)
        grad_c = grad_c + dot_nt(grow_g, ent_ref[0, 0, :, at])
        lasts = jnp.sum(aft_ref[0, 0, :, at] * ds_old, axis=0, keepdims=True)
        dlast = dlast + split_dot(jnp.broadcast_to(lasts, (8, LANES)), seg)
        state[:, at] = ds_old * pair_of(decay, i, low) + (dot(c_t, grow_g) + dot(c_t, grow_lo))
        zero = jnp.zeros_like(xdt_b)
        tops = jnp.zeros((half, LANES), F32)
        bots = jnp.zeros((half, LANES), F32)
        for s in range(2):
            h = 2 * i + s
            xm = jnp.where(low, xdt_b, zero) if s == 0 else jnp.where(low, zero, xdt_b)
            gs = jnp.where(low, gm_b, zero) if s == 0 else jnp.where(low, zero, gm_b)
            gl = jnp.where(low, gm_lo, zero) if s == 0 else jnp.where(low, zero, gm_lo)
            row, col = cum_t[h : h + 1, :], cum[:, h : h + 1]
            low_a = jnp.exp(row[:, :half] - col[:half] + mask)
            low_b = jnp.exp(row[:, half:] - col[:half])
            low_d = jnp.exp(row[:, half:] - col[half:] + mask)
            dm_top = dot_nt(xm[:half], gm_b)
            dm_bot = dot_nt(xm[half:], gm_b[half:])
            ds_a = ds_a + dm_top[:, :half] * low_a
            ds_b = ds_b + dm_top[:, half:] * low_b
            ds_d = ds_d + dm_bot * low_d
            mix = jnp.concatenate(
                [
                    (low_a * scores_t[:half, :half]).astype(BF),
                    (low_b * scores_t[:half, half:]).astype(BF),
                ],
                axis=1,
            )
            tops = tops + (dot(mix, gs) + dot(mix, gl))
            mix = (low_d * scores_t[half:, half:]).astype(BF)
            bots = bots + (dot(mix, gs[half:]) + dot(mix, gl[half:]))
        dxdt = dxdt + jnp.concatenate([tops, bots], axis=0)
        skip = chan_ref[0:1, at]
        dcum = dcum + split_dot(gm * (mixed_ref[0, :, at] - skip * x), seg)
        cols = cols + split_dot(xdt * dxdt, seg)
        gx = (dt_e * dxdt + skip * gm) * dsx_ref[0, :, at].astype(F32)
        ext_x[0:L, at] = gx
        px = px_ref[0, :, at]
        cot = cx_ref[3:4, at] * gx
        sx_ref[3:4, at] = sx_ref[3:4, at] + jnp.sum(px * gx, axis=0, keepdims=True)
        sx_ref[4:5, at] = sx_ref[4:5, at] + jnp.sum(gx, axis=0, keepdims=True)
        for k in range(3):
            moved = ext_x[3 - k : 3 - k + L, at]
            cot = cot + cx_ref[k : k + 1, at] * moved
            sx_ref[k : k + 1, at] = sx_ref[k : k + 1, at] + jnp.sum(
                px * moved, axis=0, keepdims=True
            )
        cot_ref[0, :, at] = cgate_ref[0, :, at]
        cot_ref[0, :, width + i * LANES : width + (i + 1) * LANES] = cot.astype(BF)

    zero = jnp.zeros((half, half), F32)
    ds_t = jnp.concatenate(
        [jnp.concatenate([ds_a, ds_b], axis=1), jnp.concatenate([zero, ds_d], axis=1)], axis=0
    )
    grad_b = grad_b + dot(ds_t.astype(BF), c)
    grad_c = grad_c + dot(ds_t.T.astype(BF), b)
    for i, part in ((0, grad_b), (1, grad_c)):
        at = slice(i * LANES, (i + 1) * LANES)
        gb = part * dsbc_ref[0, :, at].astype(F32)
        ext_bc[0:L, at] = gb
        pb = pbc_ref[0, :, at]
        cot = cbc_ref[3:4, at] * gb
        sbc_ref[3:4, at] = sbc_ref[3:4, at] + jnp.sum(pb * gb, axis=0, keepdims=True)
        sbc_ref[4:5, at] = sbc_ref[4:5, at] + jnp.sum(gb, axis=0, keepdims=True)
        for k in range(3):
            moved = ext_bc[3 - k : 3 - k + L, at]
            cot = cot + cbc_ref[k : k + 1, at] * moved
            sbc_ref[k : k + 1, at] = sbc_ref[k : k + 1, at] + jnp.sum(
                pb * moved, axis=0, keepdims=True
            )
        cot_ref[0, :, 2 * width + i * LANES : 2 * width + (i + 1) * LANES] = cot.astype(BF)

    upper = jnp.where(iota((L, L), 1) >= iota((L, L), 0), 1.0, 0.0).astype(BF)
    drate = dot_split(upper, dcum - cols) + dlast[0:1, :]
    z = pdt_ref[0] + small_ref[0:1, :]
    sig = sigmoid(z)
    ratio = jnp.where(z < -15.0, 1.0, sig / jnp.where(z < -15.0, 1.0, step))
    dz = cols * ratio + drate * small_ref[1:2, :] * sig
    cot_ref[0, :, 2 * width + 2 * LANES : 2 * width + 3 * LANES] = dz.astype(BF)
    sdt_ref[0:1, :] = sdt_ref[0:1, :] + jnp.sum(dz, axis=0, keepdims=True)
    sdt_ref[1:2, :] = sdt_ref[1:2, :] + jnp.sum(
        drate * step * small_ref[1:2, :], axis=0, keepdims=True
    )

    @pl.when(g == final)
    def _():
        for ext, taps, sums, first, wide in (
            (ext_x, cx_ref, sx_ref, 0, width),
            (ext_bc, cbc_ref, sbc_ref, width, 2 * LANES),
        ):
            both = jnp.concatenate([jnp.zeros((8, wide), F32), ext[0:8, :]], axis=0)
            before = halo_ref[0, :, first : first + wide]
            total = jnp.zeros((8, wide), F32)
            for k in range(3):
                moved = both[3 - k : 11 - k, :]
                total = total + taps[k : k + 1, :] * moved
                sums[k : k + 1, :] = sums[k : k + 1, :] + jnp.sum(
                    before * moved, axis=0, keepdims=True
                )
            tail_ref[0, :, first : first + wide] = total
        tail_ref[0, :, width + 2 * LANES :] = jnp.zeros((8, LANES), F32)

    ext_x[L : L + 8, :] = ext_x[0:8, :]
    ext_bc[L : L + 8, :] = ext_bc[0:8, :]


def tensor_peers():
    me = lax.axis_index("tensor")
    chip, core = me // 2, lax.rem(me, 2)
    partner = chip * 2 + (1 - core)
    across = (1 - chip) * 2 + core
    return me, chip, core, partner, across


def greet(partner, across):
    barrier = pltpu.get_barrier_semaphore()
    for peer in (partner, across):
        pl.semaphore_signal(barrier, inc=1, device_id={"tensor": peer}, device_id_type=MESH)
    pl.semaphore_wait(barrier, 2)


def gather_kernel(cuts, count, *refs):
    ins, outs = refs[:count], refs[count : 2 * count]
    own_sem, near_s, near_r, far_s, far_r, pass_s, pass_r = refs[2 * count :]
    me, chip, core, partner, across = tensor_peers()
    greet(partner, across)
    batch, rows = ins[0].shape[0], ins[0].shape[1]
    piece = rows // cuts

    def remote(src, dst, send, recv, peer):
        return pltpu.make_async_remote_copy(
            src_ref=src,
            dst_ref=dst,
            send_sem=send,
            recv_sem=recv,
            device_id={"tensor": peer},
            device_id_type=MESH,
        )

    todo = []
    at = 0
    for a in range(count):
        for n in range(batch):
            for cut in range(cuts):
                mine = pl.ds(pl.multiple_of(me * rows + cut * piece, piece), piece)
                theirs = pl.ds(pl.multiple_of(across * rows + cut * piece, piece), piece)
                src = ins[a].at[n, cut * piece : (cut + 1) * piece, :]
                far = remote(src, outs[a].at[n, mine, :], far_s.at[at], far_r.at[at], across)
                near = remote(src, outs[a].at[n, mine, :], near_s.at[at], near_r.at[at], partner)
                own = pltpu.make_async_copy(src, outs[a].at[n, mine, :], own_sem.at[at])
                here = outs[a].at[n, theirs, :]
                onward = remote(here, here, pass_s.at[at], pass_r.at[at], partner)
                todo.append((far, near, own, onward))
                at += 1
    for far, near, own, onward in todo:
        far.start()
    for far, near, own, onward in todo:
        near.start()
        own.start()
    for far, near, own, onward in todo:
        far.wait_recv()
        onward.start()
    for far, near, own, onward in todo:
        far.wait_send()
        near.wait()
        own.wait()
        onward.wait()


def gather_tokens(*arrays):
    size = lax.axis_size("tensor")
    if size != 4:
        return [lax.all_gather(a, "tensor", axis=1, tiled=True) for a in arrays]
    batch, rows, width = arrays[0].shape
    count, cuts = len(arrays), 2
    sems = count * batch * cuts
    out = jax.ShapeDtypeStruct((batch, size * rows, width), arrays[0].dtype)
    return pl.pallas_call(
        functools.partial(gather_kernel, cuts, count),
        out_shape=[out] * count,
        in_specs=[pl.BlockSpec(memory_space=pltpu.VMEM)] * count,
        out_specs=[pl.BlockSpec(memory_space=pl.ANY)] * count,
        scratch_shapes=[pltpu.SemaphoreType.DMA((sems,))] * 7,
        compiler_params=pltpu.CompilerParams(
            collective_id=0, has_side_effects=True, vmem_limit_bytes=16 * 1024 * 1024
        ),
        name="gather_tokens",
    )(*arrays)


def scatter_kernel(cuts, in_ref, out_ref, near_buf, far_buf, sum_buf, near_s, near_r, far_s, far_r):
    me, chip, core, partner, across = tensor_peers()
    greet(partner, across)
    batch, rows = out_ref.shape[0], out_ref.shape[1]
    piece = rows // cuts

    def rows_of(owner, cut):
        return pl.ds(pl.multiple_of(owner * rows + cut * piece, piece), piece)

    def remote(src, dst, send, recv, peer):
        return pltpu.make_async_remote_copy(
            src_ref=src,
            dst_ref=dst,
            send_sem=send,
            recv_sem=recv,
            device_id={"tensor": peer},
            device_id_type=MESH,
        )

    near = {}
    for step, target in ((0, (1 - chip) * 2 + (1 - core)), (1, chip * 2 + (1 - core))):
        for n in range(batch):
            for cut in range(cuts):
                at = (step * batch + n) * cuts + cut
                near[step, n, cut] = remote(
                    in_ref.at[n, rows_of(target, cut), :],
                    near_buf.at[at],
                    near_s.at[at],
                    near_r.at[at],
                    partner,
                )
                near[step, n, cut].start()
    far = {}
    for n in range(batch):
        for cut in range(cuts):
            at = n * cuts + cut
            near[0, n, cut].wait_recv()
            sum_buf[at] = (
                in_ref[n, rows_of(across, cut), :].astype(F32) + near_buf[at].astype(F32)
            ).astype(BF)
            far[n, cut] = remote(
                sum_buf.at[at], far_buf.at[at], far_s.at[at], far_r.at[at], across
            )
            far[n, cut].start()
    for n in range(batch):
        for cut in range(cuts):
            at = n * cuts + cut
            near[1, n, cut].wait_recv()
            far[n, cut].wait_recv()
            out_ref[n, cut * piece : (cut + 1) * piece, :] = (
                in_ref[n, rows_of(me, cut), :].astype(F32)
                + near_buf[batch * cuts + at].astype(F32)
                + far_buf[at].astype(F32)
            )
    for key in near:
        near[key].wait_send()
    for key in far:
        far[key].wait_send()


def scatter_tokens(part, ident):
    size = lax.axis_size("tensor")
    if size != 4:
        return lax.psum_scatter(part, "tensor", scatter_dimension=1, tiled=True).astype(F32)
    batch, tokens, width = part.shape
    rows, cuts = tokens // size, 2
    piece = rows // cuts
    return pl.pallas_call(
        functools.partial(scatter_kernel, cuts),
        out_shape=jax.ShapeDtypeStruct((batch, rows, width), F32),
        in_specs=[pl.BlockSpec(memory_space=pltpu.VMEM)],
        out_specs=pl.BlockSpec(memory_space=pltpu.VMEM),
        scratch_shapes=[
            pltpu.VMEM((2 * batch * cuts, piece, width), BF),
            pltpu.VMEM((batch * cuts, piece, width), BF),
            pltpu.VMEM((batch * cuts, piece, width), BF),
            pltpu.SemaphoreType.DMA((2 * batch * cuts,)),
            pltpu.SemaphoreType.DMA((2 * batch * cuts,)),
            pltpu.SemaphoreType.DMA((batch * cuts,)),
            pltpu.SemaphoreType.DMA((batch * cuts,)),
        ],
        compiler_params=pltpu.CompilerParams(
            collective_id=ident, has_side_effects=True, vmem_limit_bytes=40 * 1024 * 1024
        ),
        name="scatter_tokens",
    )(part)


def chain_kernel(by, cuts, own_ref, tot_ref, out_ref, in_buf, send_buf, send_sem, recv_sem):
    me, size = lax.axis_index("seq"), lax.axis_size("seq")
    ahead, behind = me + by, me - by
    has_next = (ahead >= 0) & (ahead < size)
    has_prev = (behind >= 0) & (behind < size)
    barrier = pltpu.get_barrier_semaphore()

    @pl.when(has_next)
    def _():
        pl.semaphore_signal(barrier, inc=1, device_id={"seq": ahead}, device_id_type=MESH)

    @pl.when(has_prev)
    def _():
        pl.semaphore_signal(barrier, inc=1, device_id={"seq": behind}, device_id_type=MESH)

    pl.semaphore_wait(barrier, has_next.astype(jnp.int32) + has_prev.astype(jnp.int32))

    batch, rows = own_ref.shape[0], own_ref.shape[1] // cuts
    copies = []
    for n in range(batch):
        decay = jnp.exp(tot_ref[n, 0:1, :])
        for cut in range(cuts):
            at = n * cuts + cut
            here = slice(cut * rows, (cut + 1) * rows)
            copy = pltpu.make_async_remote_copy(
                src_ref=send_buf.at[at],
                dst_ref=in_buf.at[at],
                send_sem=send_sem.at[at],
                recv_sem=recv_sem.at[at],
                device_id={"seq": ahead},
                device_id_type=MESH,
            )
            copies.append(copy)

            @pl.when(has_prev)
            def _():
                copy.wait_recv()
                out_ref[n, here, :] = in_buf[at].astype(F32)

            @pl.when(jnp.logical_not(has_prev))
            def _():
                out_ref[n, here, :] = jnp.zeros((rows, out_ref.shape[2]), F32)

            @pl.when(has_next)
            def _():
                send_buf[at] = (out_ref[n, here, :] * decay + own_ref[n, here, :]).astype(BF)
                copy.start()

    @pl.when(has_next)
    def _():
        for copy in copies:
            copy.wait_send()


def chain(own, tot, by, ident):
    batch, rows, width = own.shape
    cuts = 4
    return pl.pallas_call(
        functools.partial(chain_kernel, by, cuts),
        out_shape=jax.ShapeDtypeStruct(own.shape, F32),
        in_specs=[pl.BlockSpec(memory_space=pltpu.VMEM)] * 2,
        out_specs=pl.BlockSpec(memory_space=pltpu.VMEM),
        scratch_shapes=[
            pltpu.VMEM((batch * cuts, rows // cuts, width), BF),
            pltpu.VMEM((batch * cuts, rows // cuts, width), BF),
            pltpu.SemaphoreType.DMA((batch * cuts,)),
            pltpu.SemaphoreType.DMA((batch * cuts,)),
        ],
        compiler_params=pltpu.CompilerParams(collective_id=ident, has_side_effects=True),
        name="chain",
    )(own, tot)


def sum_kernel(phases, in_ref, out_ref, *scratch):
    count = len(phases)
    bufs, sends, recvs = scratch[:count], scratch[count : 2 * count], scratch[2 * count :]
    barrier = pltpu.get_barrier_semaphore()
    greeted = 0
    for axis, _, _ in phases:
        me, size = lax.axis_index(axis), lax.axis_size(axis)
        for d in range(1, size):
            peer = lax.rem(me + d, size)
            pl.semaphore_signal(barrier, inc=1, device_id={axis: peer}, device_id_type=MESH)
            greeted += 1
    pl.semaphore_wait(barrier, greeted)
    out_ref[...] = in_ref[...]
    for p, (axis, first, stop) in enumerate(phases):
        me, size = lax.axis_index(axis), lax.axis_size(axis)
        rows = stop - first
        bufs[p][pl.ds(me, 1)] = out_ref[first:stop, :].reshape(1, rows, LANES)
        copies = []
        for d in range(1, size):
            copies.append(
                pltpu.make_async_remote_copy(
                    src_ref=(in_ref if p == 0 else out_ref).at[pl.ds(first, rows), :],
                    dst_ref=bufs[p].at[me],
                    send_sem=sends[p].at[d - 1],
                    recv_sem=recvs[p].at[d - 1],
                    device_id={axis: lax.rem(me + d, size)},
                    device_id_type=MESH,
                )
            )
            copies[-1].start()
        for copy in copies:
            copy.wait()
        total = bufs[p][0]
        for r in range(1, size):
            total = total + bufs[p][r]
        out_ref[first:stop, :] = total


def small_sum(value, phases, ident):
    sizes = [lax.axis_size(axis) for axis, _, _ in phases]
    scratch = [
        pltpu.VMEM((n, stop - first, LANES), F32) for n, (_, first, stop) in zip(sizes, phases)
    ]
    scratch += [pltpu.SemaphoreType.DMA((max(n - 1, 1),)) for n in sizes] * 2
    return pl.pallas_call(
        functools.partial(sum_kernel, phases),
        out_shape=jax.ShapeDtypeStruct(value.shape, F32),
        in_specs=[pl.BlockSpec(memory_space=pltpu.VMEM)],
        out_specs=pl.BlockSpec(memory_space=pltpu.VMEM),
        scratch_shapes=scratch,
        compiler_params=pltpu.CompilerParams(collective_id=ident, has_side_effects=True),
        name="small_sum",
    )(value)


def rows_of_lanes(flat, unit=8 * LANES):
    short = -flat.shape[0] % unit
    return jnp.pad(flat, (0, short)).reshape(-1, LANES)


def shifted(value, by):
    peers = lax.axis_size("seq")
    pairs = [(i, i + by) for i in range(peers) if 0 <= i + by < peers]
    return lax.ppermute(value, "seq", pairs)


def pad_last(value, to):
    short = to - value.shape[-1]
    if short == 0:
        return value
    return jnp.pad(value, [(0, 0)] * (value.ndim - 1) + [(0, short)])


def token_spec(width, col=0, flip=None):
    if flip is None:
        return pl.BlockSpec((1, L, width), lambda n, j: (n, j, col))
    return pl.BlockSpec((1, L, width), lambda n, j: (n, flip - 1 - j, col))


def span_spec(shape):
    return pl.BlockSpec((1,) + shape, lambda n, j: (n,) + (0,) * len(shape))


def whole_spec(shape):
    return pl.BlockSpec(shape, lambda n, j: (0,) * len(shape))


def shards(
    block_input,
    gain_in,
    w_zx,
    w_bc,
    w_dt,
    conv_x,
    conv_x_b,
    conv_bc,
    conv_bc_b,
    dt_bias,
    a_log,
    d_skip,
    gain_norm,
    w_out,
    cotangent,
):
    rows_dev, batch, model = block_input.shape
    tensor_count = lax.axis_size("tensor")
    span = rows_dev * tensor_count
    groups = span // L
    heads = dt_bias.shape[0]
    inner = gain_norm.shape[0]
    inner_total = inner * tensor_count
    state_n = conv_bc.shape[2]
    pairs = (heads + 1) // 2
    width = pairs * LANES
    tails = width + 3 * LANES
    wide = width + tails
    rows_w = w_out.shape[0]
    pspace = ("dp", "seq")

    mine_in = jnp.concatenate(
        [
            pad_last(w_zx[:, 0], width),
            pad_last(w_zx[:, 1], width),
            w_bc.reshape(rows_w, 2 * state_n),
            pad_last(w_dt, LANES),
        ],
        axis=1,
    )
    mine_o = pad_last(w_out, width)
    full_in = lax.all_gather(mine_in, pspace, axis=0, tiled=True)
    full_in, mine_o = lax.optimization_barrier((full_in, mine_o))
    full_o = lax.all_gather(mine_o, pspace, axis=0, tiled=True)

    flat_in = jnp.swapaxes(block_input, 0, 1).astype(F32)
    cot_rows = jnp.swapaxes(cotangent, 0, 1)
    inv_in = lax.rsqrt(jnp.mean(flat_in * flat_in, -1, keepdims=True) + EPS)
    base = flat_in * inv_in
    normed_rows = (base * gain_in).astype(BF)
    normed, cots = gather_tokens(normed_rows, cot_rows)
    halo_rows = shifted(normed[:, span - 8 :], 1)

    taps_x = pad_last(jnp.concatenate([conv_x, conv_x_b[None], jnp.zeros((3, inner), F32)], 0), width)
    taps_bc = jnp.concatenate(
        [
            conv_bc.reshape(4, 2 * state_n),
            conv_bc_b.reshape(1, 2 * state_n),
            jnp.zeros((3, 2 * state_n), F32),
        ],
        0,
    )
    small = pad_last(jnp.stack([dt_bias, -jnp.exp(a_log)] + [jnp.zeros_like(a_log)] * 6), LANES)
    chan = pad_last(
        jnp.stack([jnp.repeat(d_skip, HD), gain_norm] + [jnp.zeros_like(gain_norm)] * 6), width
    )

    pre = jnp.einsum("btd,dk->btk", normed, full_in, preferred_element_type=F32)
    halo = jnp.einsum("btd,dk->btk", halo_rows, full_in[:, width:], preferred_element_type=F32)
    grad_hidden = jnp.einsum("btd,dk->btk", cots, full_o, preferred_element_type=F32)

    params = pltpu.CompilerParams(
        dimension_semantics=("arbitrary", "arbitrary"), vmem_limit_bytes=VMEM_LIMIT
    )
    grid = (batch, groups)
    at_bc, at_dt = pairs, 2 * pairs + 2
    sds = jax.ShapeDtypeStruct
    x_act, ds_x, bc_act, ds_bc, step, cum, local_state, tot = pl.pallas_call(
        functools.partial(acts_kernel, pairs),
        grid=grid,
        out_shape=[
            sds((batch, span, width), F32),
            sds((batch, span, width), BF),
            sds((batch, span, 2 * LANES), F32),
            sds((batch, span, 2 * LANES), BF),
            sds((batch, span, LANES), F32),
            sds((batch, span, LANES), F32),
            sds((batch, LANES, width), F32),
            sds((batch, 8, LANES), F32),
        ],
        in_specs=[
            token_spec(width, 1),
            token_spec(2 * LANES, at_bc),
            token_spec(LANES, at_dt),
            span_spec((8, tails)),
            whole_spec((8, width)),
            whole_spec((8, 2 * LANES)),
            whole_spec((8, LANES)),
        ],
        out_specs=[
            token_spec(width),
            token_spec(width),
            token_spec(2 * LANES),
            token_spec(2 * LANES),
            token_spec(LANES),
            token_spec(LANES),
            span_spec((LANES, width)),
            span_spec((8, LANES)),
        ],
        scratch_shapes=[pltpu.VMEM((L + 8, width), F32), pltpu.VMEM((L + 8, 2 * LANES), F32)],
        compiler_params=params,
        name="acts",
    )(pre, pre, pre, halo, taps_x, taps_bc, small)

    tot_wide = jnp.repeat(tot[:, :, : 2 * pairs], HD, axis=-1)
    state_in = chain(local_state, tot_wide, 1, 3)

    mixed, ent, aft, stats = pl.pallas_call(
        functools.partial(forward_kernel, pairs),
        grid=grid,
        out_shape=[
            sds((batch, span, width), F32),
            sds((batch, groups, LANES, width), BF),
            sds((batch, groups, LANES, width), F32),
            sds((batch, 2, span), F32),
        ],
        in_specs=[
            token_spec(width),
            token_spec(2 * LANES),
            token_spec(LANES),
            token_spec(LANES),
            token_spec(width),
            token_spec(width),
            span_spec((LANES, width)),
            whole_spec((8, width)),
        ],
        out_specs=[
            token_spec(width),
            pl.BlockSpec((1, 1, LANES, width), lambda n, j: (n, j, 0, 0)),
            pl.BlockSpec((1, 1, LANES, width), lambda n, j: (n, j, 0, 0)),
            pl.BlockSpec((1, 2, L), lambda n, j: (n, 0, j)),
        ],
        scratch_shapes=[pltpu.VMEM((LANES, width), F32)],
        compiler_params=params,
        name="ssd_forward",
    )(x_act, bc_act, step, cum, pre, grad_hidden, state_in, chan)

    rows = stats.size // LANES
    stats = small_sum(stats.reshape(rows, LANES), (("tensor", 0, rows),), 4).reshape(stats.shape)

    grad_mixed, cot_gate, hidden, ds_local, sums_n = pl.pallas_call(
        functools.partial(gating_kernel, pairs, inner_total),
        grid=grid,
        out_shape=[
            sds((batch, span, width), F32),
            sds((batch, span, width), BF),
            sds((batch, span, width), BF),
            sds((batch, LANES, width), F32),
            sds((8, width), F32),
        ],
        in_specs=[
            token_spec(width),
            token_spec(2 * LANES),
            token_spec(LANES),
            token_spec(width),
            token_spec(width),
            token_spec(width),
            pl.BlockSpec((1, 2, L), lambda n, j: (n, 0, j)),
            whole_spec((8, width)),
        ],
        out_specs=[
            token_spec(width),
            token_spec(width),
            token_spec(width),
            span_spec((LANES, width)),
            whole_spec((8, width)),
        ],
        scratch_shapes=[pltpu.VMEM((8, LANES), F32)],
        compiler_params=params,
        name="gating_backward",
    )(x_act, bc_act, cum, pre, grad_hidden, mixed, stats, chan)

    carried = chain(ds_local, tot_wide, -1, 5)

    grad_o = jnp.einsum("btd,btk->dk", cots, hidden, preferred_element_type=F32).astype(BF)
    grad_z = jnp.einsum("btd,btk->dk", normed, cot_gate, preferred_element_type=F32).astype(BF)
    grad_oz = with_layout_constraint(
        jnp.concatenate([grad_o, grad_z], axis=1), Layout(major_to_minor=(0, 1))
    )
    carried, grad_oz, hidden = lax.optimization_barrier((carried, grad_oz, hidden))
    red_oz = lax.psum_scatter(grad_oz, pspace, scatter_dimension=0, tiled=True)
    branch_part = jnp.einsum("btk,dk->btd", hidden, full_o, preferred_element_type=F32).astype(BF)
    branch = scatter_tokens(branch_part, 1)
    carried, branch = lax.optimization_barrier((carried, branch))
    block_output = jnp.swapaxes((flat_in + branch).astype(BF), 0, 1)

    cot_in, tail, sums_x, sums_bc, sums_dt = pl.pallas_call(
        functools.partial(backward_kernel, pairs),
        grid=grid,
        out_shape=[
            sds((batch, span, wide), BF),
            sds((batch, 8, tails), F32),
            sds((8, width), F32),
            sds((8, 2 * LANES), F32),
            sds((8, LANES), F32),
        ],
        in_specs=[
            token_spec(width, 0, groups),
            token_spec(width, 0, groups),
            token_spec(width, 0, groups),
            token_spec(width, 0, groups),
            token_spec(2 * LANES, 0, groups),
            token_spec(2 * LANES, 0, groups),
            token_spec(LANES, 0, groups),
            token_spec(LANES, 0, groups),
            pl.BlockSpec((1, 1, LANES, width), lambda n, j: (n, groups - 1 - j, 0, 0)),
            pl.BlockSpec((1, 1, LANES, width), lambda n, j: (n, groups - 1 - j, 0, 0)),
            token_spec(width, 0, groups),
            token_spec(width, 1, groups),
            token_spec(2 * LANES, at_bc, groups),
            token_spec(LANES, at_dt, groups),
            span_spec((8, tails)),
            span_spec((LANES, width)),
            whole_spec((8, width)),
            whole_spec((8, width)),
            whole_spec((8, 2 * LANES)),
            whole_spec((8, LANES)),
        ],
        out_specs=[
            token_spec(wide, 0, groups),
            span_spec((8, tails)),
            whole_spec((8, width)),
            whole_spec((8, 2 * LANES)),
            whole_spec((8, LANES)),
        ],
        scratch_shapes=[
            pltpu.VMEM((LANES, width), F32),
            pltpu.VMEM((L + 8, width), F32),
            pltpu.VMEM((L + 8, 2 * LANES), F32),
        ],
        compiler_params=params,
        name="ssd_backward",
    )(
        grad_mixed,
        cot_gate,
        x_act,
        ds_x,
        bc_act,
        ds_bc,
        step,
        cum,
        ent,
        aft,
        mixed,
        pre,
        pre,
        pre,
        halo,
        carried,
        chan,
        taps_x,
        taps_bc,
        small,
    )
    later = shifted(tail, -1)
    cot_in = cot_in.at[:, span - 8 :, width:].add(later.astype(BF))

    grad_wx = jnp.einsum("btd,btk->dk", normed, cot_in[..., width:], preferred_element_type=F32)
    grad_wx, cot_in, red_oz = lax.optimization_barrier((grad_wx.astype(BF), cot_in, red_oz))
    red_x = lax.psum_scatter(grad_wx, pspace, scatter_dimension=0, tiled=True)
    part = jnp.einsum("btk,dk->btd", cot_in, full_in, preferred_element_type=F32).astype(BF)
    grad_normed = scatter_tokens(part, 2)

    scaled = grad_normed * gain_in
    grad_base = inv_in * (scaled - base * jnp.mean(scaled * base, -1, keepdims=True))
    input_grad = jnp.swapaxes((cot_rows.astype(F32) + grad_base).astype(BF), 0, 1)
    gain_part = jnp.sum(grad_normed * base, (0, 1))

    sizes_own = (
        sums_x[:5, :inner].reshape(-1),
        sums_n[0, :inner],
        jnp.sum(sums_n[1, :inner].reshape(heads, HD), -1),
        sums_dt[0, :heads],
        sums_dt[1, :heads],
    )
    mine = rows_of_lanes(jnp.concatenate(sizes_own))
    rest = rows_of_lanes(jnp.concatenate([sums_bc[:5].reshape(-1), gain_part]))
    part_bc = red_x[:, width : width + 2 * state_n].astype(F32).reshape(-1, LANES)
    first = mine.shape[0]
    second = first + rest.shape[0]
    third = second + part_bc.shape[0]
    summed = small_sum(
        jnp.concatenate([mine, rest, part_bc], 0),
        (("dp", 0, second), ("seq", 0, second), ("tensor", first, third)),
        6,
    )
    own, shared = summed[:first].reshape(-1), summed[first:second].reshape(-1)
    grad_bc = summed[second:]

    n5 = 5 * inner
    bc5 = 5 * 2 * state_n
    return (
        block_output,
        input_grad,
        shared[bc5 : bc5 + model],
        jnp.stack([red_oz[:, width : width + inner], red_x[:, :inner]], 1).astype(F32),
        grad_bc.reshape(rows_w, 2, state_n),
        red_x[:, width + 2 * state_n : width + 2 * state_n + heads].astype(F32),
        own[: 4 * inner].reshape(4, inner),
        own[4 * inner : n5],
        shared[: 4 * 2 * state_n].reshape(4, 2, state_n),
        shared[4 * 2 * state_n : bc5].reshape(2, state_n),
        own[n5 + inner + heads : n5 + inner + 2 * heads],
        own[n5 + inner + 2 * heads : n5 + inner + 3 * heads],
        own[n5 + inner : n5 + inner + heads],
        own[n5 : n5 + inner],
        red_oz[:, :inner].astype(F32),
    )


def solution(mesh):
    return jax.shard_map(
        shards,
        mesh=mesh,
        in_specs=(
            P(("seq", "tensor"), "dp", None),
            P(),
            P(("dp", "seq"), None, "tensor"),
            P(("dp", "seq"), None, None),
            P(("dp", "seq"), "tensor"),
            P(None, "tensor"),
            P("tensor"),
            P(),
            P(),
            P("tensor"),
            P("tensor"),
            P("tensor"),
            P("tensor"),
            P(("dp", "seq"), "tensor"),
            P(("seq", "tensor"), "dp", None),
        ),
        out_specs=(
            P(("seq", "tensor"), "dp", None),
            P(("seq", "tensor"), "dp", None),
            P(),
            P(("dp", "seq"), None, "tensor"),
            P(("dp", "seq"), None, None),
            P(("dp", "seq"), "tensor"),
            P(None, "tensor"),
            P("tensor"),
            P(),
            P(),
            P("tensor"),
            P("tensor"),
            P("tensor"),
            P("tensor"),
            P(("dp", "seq"), "tensor"),
        ),
        check_vma=False,
    )
```
